32 devices in a mesh: blk: 8 (over z, y), head: 4 (over x, core).
Axes of the slice: x: 2, y: 2, z: 4, core: 2. Of those that a mesh axis runs over, the one named last changes fastest.
Arguments:
- queries: bfloat16 [4096, 1024], P('blk', 'head'), may hold values from -170 to 170
- key_rows: bfloat16 [4096, 1024], P('blk', 'head'), may hold values from -9 to 9
- values: bfloat16 [4096, 1024], P('blk', 'head'), may hold values from -48 to 48
- text_keys: bfloat16 [308, 1024], P(None, 'head'), may hold values from -9 to 9
- text_values: bfloat16 [308, 1024], P(None, 'head'), may hold values from -48 to 48
- block_image: int32 [32], replicated, may hold values from 0 to 1, as said below
- gate_image: float32 [2, 1536], replicated, may hold values from 0.5 to 2
- residual: bfloat16 [4096, 1536], P(('blk', 'head')), may hold values from -6 to 6
- w_out: bfloat16 [1024, 1536], P('head'), may hold values from -0.1875 to 0.1875
Outputs:
- stream_out: bfloat16 [4096, 1536], P(('blk', 'head'))
The draws below stay inside these ranges and needn't reach their ends.
Inputs may be any that keep to these rules, and one draw needn't show every extreme that they name: `block_image`: each image number 0 to 1 names 8 to 24 of the entries, some image exactly 24 and some exactly 8; the blocks of an image lie anywhere in the array.
All inputs are finite; a program needn't handle non-finite values.
Results may differ from the reference program's by a relative error of at most 0.014.
Values may be sent and summed in bfloat16 or wider, within the bound.
A program may use at most 64 MiB of HBM per device.

```python
import math
import jax
import jax.numpy as jnp
from jax import lax

D = 1536
HEADS = 16
HD = 64
TEXT = 154
BS = 128
TOK_BLK = 512
NBLOCKS = 32
IMAGES = 2
TOKENS = 4096


def shared_keys(key):
    base = 1.5 * jax.random.normal(jax.random.fold_in(key, 7), (TOKENS, HEADS * HD), jnp.float32)
    base = jnp.clip(base, -9.0, 9.0)
    return base


def draw_key_rows(key, part):
    base = shared_keys(key)
    return base.astype(jnp.bfloat16)


def draw_queries(key, part):
    fresh = 1.5 * jax.random.normal(jax.random.fold_in(key, 9), (TOKENS, HEADS * HD), jnp.float32)
    fresh = jnp.clip(fresh, -9.0, 9.0)
    return fresh.astype(jnp.bfloat16)


def draw_block_image(key, part):
    pairs = IMAGES // 2
    split = jax.random.randint(jax.random.fold_in(key, 1), (pairs,), 8, 25)
    split = split.at[0].set(24)
    counts = jnp.stack([split, 32 - split], axis=1).reshape(IMAGES)
    labels = jax.random.permutation(jax.random.fold_in(key, 2), IMAGES).astype(jnp.int32)
    bounds = jnp.cumsum(counts)
    blocks = jnp.arange(NBLOCKS)
    sorted_slot = jnp.sum((blocks[:, None] >= bounds[None, :]).astype(jnp.int32), axis=1)
    image = labels[sorted_slot]
    order = jax.random.permutation(jax.random.fold_in(key, 3), NBLOCKS)
    return image[order].astype(jnp.int32)


def shard_levels(key, extent, shards, smallest, high):
    loudness = 1.0
    for position, blocks in shards:
        steps = jax.random.uniform(jax.random.fold_in(jax.random.fold_in(key, 6), position), (blocks,), jnp.float32, smallest / len(shards), high / len(shards))
        loudness = loudness * jnp.repeat(jnp.exp(steps), extent[position] // blocks).reshape((-1,) + (1,) * (len(extent) - 1 - position))
    return loudness


def centred(rng, extent, spread, reach, cuts=(), kind=jnp.bfloat16):
    values = spread * jax.random.normal(rng, extent, jnp.float32)
    if cuts:
        values = values * shard_levels(rng, extent, cuts, -0.22, 0.18)
    return jnp.clip(values, -reach, reach).astype(kind)


def setup_inputs(seed: int = 0) -> dict:
    splits = jax.random.split(jax.random.key(seed), 10)
    queries = draw_queries(jax.random.fold_in(splits[9], 71), 0)
    key_rows = draw_key_rows(jax.random.fold_in(splits[9], 71), 0)
    values = centred(splits[2], (TOKENS, HEADS * HD), 8.0, 48.0, ((0, 8), (1, 4)))
    text_keys = centred(splits[3], (IMAGES * TEXT, HEADS * HD), 1.5, 9.0, ((1, 4),))
    text_values = centred(splits[4], (IMAGES * TEXT, HEADS * HD), 8.0, 48.0, ((1, 4),))
    block_image = draw_block_image(jax.random.fold_in(splits[9], 71), 0)
    gate_image = jnp.clip(jax.random.uniform(splits[6], (IMAGES, D), jnp.float32, 0.5, 2.0), 0.5, 2.0)
    residual = centred(splits[7], (TOKENS, D), 1.0, 6.0, ((0, 32),))
    w_out = centred(splits[8], (HEADS * HD, D), (HEADS * HD) ** -0.5, 0.1875, ((0, 4),))
    return dict(queries=queries, key_rows=key_rows, values=values, text_keys=text_keys, text_values=text_values, block_image=block_image, gate_image=gate_image, residual=residual, w_out=w_out)


def reference(queries, key_rows, values, text_keys, text_values, block_image, gate_image, residual, w_out):
    token_image = jnp.repeat(block_image, BS).astype(jnp.int32)
    text_image = (jnp.arange(IMAGES * TEXT) // TEXT).astype(jnp.int32)
    every_key = jnp.concatenate([key_rows, text_keys], axis=0)
    every_value = jnp.concatenate([values, text_values], axis=0)
    key_image = jnp.concatenate([token_image, text_image], axis=0)
    scale = 1.0 / math.sqrt(HD)
    nkeys = every_key.shape[0]
    query_heads = queries.reshape(TOKENS, HEADS, HD).transpose(1, 0, 2)
    key_heads = every_key.reshape(nkeys, HEADS, HD).transpose(1, 0, 2)
    value_heads = every_value.reshape(nkeys, HEADS, HD).transpose(1, 0, 2)
    query_blocks = query_heads.reshape(HEADS, TOKENS // TOK_BLK, TOK_BLK, HD)
    image_blocks = token_image.reshape(TOKENS // TOK_BLK, TOK_BLK)

    def one_head(operands):
        qhead, khead, vhead = operands

        def one_block(inner):
            qblock, qimage = inner
            scores = jnp.dot(qblock, khead.T, preferred_element_type=jnp.float32) * scale
            allowed = qimage[:, None] == key_image[None, :]
            scores = jnp.where(allowed, scores, -1e+30)
            peak = lax.optimization_barrier(jnp.max(scores, axis=1, keepdims=True))
            expo = jnp.exp(scores - peak)
            denom = lax.optimization_barrier(jnp.sum(expo, axis=1, keepdims=True))
            numer = jnp.dot(expo.astype(jnp.bfloat16), vhead, preferred_element_type=jnp.float32)
            return (numer / denom).astype(jnp.bfloat16)
        return lax.map(one_block, (qhead, image_blocks))
    attended = lax.map(one_head, (query_blocks, key_heads, value_heads))
    attended = attended.reshape(HEADS, TOKENS, HD).transpose(1, 0, 2).reshape(TOKENS, HEADS * HD)
    projected = jnp.dot(attended, w_out, preferred_element_type=jnp.float32)
    gating = gate_image[token_image]
    return (residual.astype(jnp.float32) + gating * projected).astype(jnp.bfloat16)
```

```python
import functools

import jax
import jax.numpy as jnp
from jax import lax
from jax.experimental import pallas as pl
from jax.experimental.pallas import tpu as pltpu
from jax.sharding import PartitionSpec as P

HD = 64
TEXT = 154
BS = 128
NEG = -1e30
LANES = 128
QTILE = 512
KEYS = 1024
MESH = pl.DeviceIdType.MESH
F32 = jnp.float32
BF16 = jnp.bfloat16


def partner(z, i):
    out, bit = z, 1
    while bit <= i:
        if i & bit:
            out = out + bit - 2 * bit * ((out // bit) % 2)
        bit *= 2
    return out


def kernel(
    n, nh, q_ref, k_ref, v_ref, tk_ref, tv_ref, img_ref, gate_ref, res_ref, w_ref, out_ref,
    qs, kvs, qr, kvr, traw, qaug, kaug, kval, taug, tval, best, accum, osend, orecv, mixed, wfull, resv,
    q_send, q_recv, kv_send, kv_recv, wx_send, ws_send, w_recv, o_send, o_recv, l_sem,
):
    tok, cols = q_ref.shape
    heads = cols // HD
    groups = n // heads
    half = tok // 2
    images = gate_ref.shape[0]
    wrows = w_ref.shape[0]
    td = res_ref.shape[0]
    texts = tk_ref.shape[0]
    per = tok // BS
    b = lax.axis_index("blk")
    j = lax.axis_index("head")
    z, r = b % heads, b // heads
    side, core = j // 2, j % 2

    barrier = pltpu.get_barrier_semaphore()
    count = 0
    for i in range(heads):
        for k in range(nh):
            if i or k:
                to = (r * heads + partner(z, i), lax.rem(j + k, nh))
                pl.semaphore_signal(barrier, inc=1, device_id=to, device_id_type=MESH)
                count += 1
    for k in range(1, groups):
        for i in range(heads):
            to = (lax.rem(r + k, groups) * heads + partner(z, i), j)
            pl.semaphore_signal(barrier, inc=1, device_id=to, device_id_type=MESH)
            count += 1

    w_here = pltpu.make_async_copy(w_ref, wfull.at[pl.ds(pl.multiple_of(j * wrows, wrows), wrows)], l_sem.at[0])
    w_here.start()
    res_here = pltpu.make_async_copy(res_ref, resv, l_sem.at[1])
    res_here.start()

    for h in range(heads):
        c = slice(h * HD, (h + 1) * HD)
        q = q_ref[:, c] * BF16(HD ** -0.5)
        qs[h] = jnp.concatenate([q[:half], q[half:]], axis=1)
        kvs[h] = jnp.concatenate([k_ref[:, c], v_ref[:, c]], axis=1)

    pl.semaphore_wait(barrier, count)

    def remote(src, dst, ss, rs, to):
        return pltpu.make_async_remote_copy(
            src_ref=src, dst_ref=dst, send_sem=ss, recv_sem=rs, device_id=to, device_id_type=MESH
        )

    sent = []

    def go(copy):
        copy.start()
        sent.append(copy)

    def wrow(owner):
        return wfull.at[pl.ds(pl.multiple_of(owner * wrows, wrows), wrows)]

    def send_kv(i, k):
        other = partner(z, i)
        pos = (groups - k) % groups * heads + i
        go(remote(kvs.at[other], kvr.at[pos], kv_send.at[pos], kv_recv.at[pos],
                  (lax.rem(r + k, groups) * heads + other, j)))

    for i in range(1, heads):
        other = partner(z, i)
        go(remote(qs.at[other], qr.at[i], q_send.at[i], q_recv.at[i], (r * heads + other, j)))
    for i in range(1, heads):
        send_kv(i, 0)
    for i in range(heads):
        for k in range(1, groups):
            send_kv(i, k)
    sib = side * 2 + 1 - core
    go(remote(w_ref, wrow(j), ws_send.at[0], w_recv.at[j], (b, sib)))
    for k in range(1, nh // 2):
        to = lax.rem(side + k, nh // 2) * 2 + core
        go(remote(w_ref, wrow(j), wx_send.at[k], w_recv.at[j], (b, to)))

    lane = lax.broadcasted_iota(jnp.int32, (16, LANES), 1)
    low_f = (lane < HD).astype(F32)
    low = low_f.astype(BF16)[:1]
    high = (1.0 - low_f).astype(BF16)[:1]

    def onehot(image):
        return jnp.where(lane == HD + image, 1.0, 0.0).astype(BF16)[:1]

    def others(image):
        return jnp.where((lane < HD) | (lane == HD + image), 0.0, NEG).astype(BF16)[:1]

    traw[...] = jnp.zeros_like(traw)
    for h in range(heads):
        c = slice(h * HD, (h + 1) * HD)

        @pl.when(z == h)
        def _():
            traw[pl.ds(0, texts), :] = jnp.concatenate([tk_ref[:, c], tv_ref[:, c]], axis=1).astype(F32)

    trow = lax.broadcasted_iota(jnp.int32, traw.shape, 0)
    tlane = lax.broadcasted_iota(jnp.int32, traw.shape, 1)
    timg = jnp.zeros_like(trow)
    for i in range(1, images + 1):
        timg += (trow >= i * TEXT).astype(jnp.int32)
    raw = traw[...]
    taug[...] = jnp.where(tlane < HD, raw, jnp.where(tlane == HD + timg, 1.0, 0.0)).astype(BF16)
    tval[...] = jnp.where(tlane < HD, 1.0, raw).astype(BF16)

    def load_q(i):
        src = qs.at[z] if i == 0 else qr.at[i]
        first = (r * heads + partner(z, i)) * per
        for p in range(per):
            at = (p * BS) % half
            x = src[pl.ds(at, BS), :]
            if p * BS >= half:
                x = pltpu.roll(x.astype(F32), HD, 1).astype(BF16)
            qaug[pl.ds(i * tok + p * BS, BS), :] = x * low + others(img_ref[first + p])

    def load_kv(pos):
        first = (lax.rem(r + pos // heads, groups) * heads + partner(z, pos % heads)) * per
        for p in range(per):
            x = kvr[pos, pl.ds(p * BS, BS), :]
            rows = pl.ds(pos * tok + p * BS, BS)
            kaug[rows, :] = x * low + onehot(img_ref[first + p])
            kval[rows, :] = x * high + low

    def absorb(keys, vals, start, count, fresh):
        def body(t, carry):
            rows = pl.ds(pl.multiple_of(start + t * QTILE, QTILE), QTILE)
            s = lax.dot_general(qaug[rows, :], keys(), (((1,), (1,)), ((), ())), preferred_element_type=F32)
            top = jnp.broadcast_to(jnp.max(s, axis=1, keepdims=True), (QTILE, LANES))
            if not fresh:
                old = best[rows, :]
                top = jnp.maximum(old, top)
            wide = jnp.concatenate([top] * (s.shape[1] // LANES), axis=1)
            p = jnp.exp(s - wide).astype(BF16)
            add = jnp.dot(p, vals(), preferred_element_type=F32)
            if fresh:
                accum[rows, :] = add
            else:
                accum[rows, :] = accum[rows, :] * jnp.exp(old - top) + add
            best[rows, :] = top
            return carry

        lax.fori_loop(0, count // QTILE, body, 0, unroll=1)

    kvr[0] = kvs[z]
    for i in range(heads):
        if i:
            remote(qs.at[0], qr.at[i], q_send.at[i], q_recv.at[i], (b, sib)).wait_recv()
        load_q(i)
        absorb(lambda: taug[...], lambda: tval[...], i * tok, tok, True)

    join = max(1, min(heads, KEYS // tok))

    def arrive(pos):
        remote(kvs.at[0], kvr.at[pos], kv_send.at[0], kv_recv.at[pos], (b, sib)).wait_recv()

    def relay_w():
        for k in range(1, nh // 2):
            owner = lax.rem(side + nh // 2 - k, nh // 2) * 2 + core
            remote(w_ref, wrow(owner), ws_send.at[k], w_recv.at[owner], (b, sib)).wait_recv()
            go(remote(wrow(owner), wrow(owner), ws_send.at[k], w_recv.at[owner], (b, sib)))

    def finish(i):
        low2 = lax.broadcasted_iota(jnp.int32, (td // 2, LANES), 1) < HD
        to_blk = r * heads + partner(z, i)
        slot = j * heads + z
        for k in range(nh):
            dest = lax.rem(j + k, nh)
            base = pl.multiple_of(i * tok + dest * td, td)
            one = accum[pl.ds(base, td // 2), :]
            two = accum[pl.ds(base + td // 2, td // 2), :]
            one_r, two_r = pltpu.roll(one, HD, 1), pltpu.roll(two, HD, 1)
            y = (jnp.where(low2, one_r, two) / jnp.where(low2, one, two_r)).astype(BF16)
            if i == 0 and k == 0:
                orecv[slot] = y
            else:
                osend[i * nh + k] = y
                go(remote(osend.at[i * nh + k], orecv.at[slot], o_send.at[i * nh + k], o_recv.at[slot],
                          (to_blk, dest)))

    for g in range(0, n, join):
        for pos in range(g, g + join):
            if pos:
                arrive(pos)
            load_kv(pos)
        at = pl.ds(g * tok, join * tok)
        args = (lambda: kaug[at, :], lambda: kval[at, :])
        if g + join == n:
            relay_w()
            for s in reversed(range(heads)):
                absorb(*args, s * tok, tok, False)
                finish(s)
        else:
            absorb(*args, 0, heads * tok, False)

    w_here.wait()
    res_here.wait()
    for k in range(nh // 2):
        owner = lax.rem(side + nh // 2 - k, nh // 2) * 2 + 1 - core
        remote(w_ref, wrow(owner), ws_send.at[k], w_recv.at[owner], (b, sib)).wait_recv()
    for i in range(heads):
        for k in range(nh):
            if i or k:
                slot = lax.rem(j + k, nh) * heads + partner(z, i)
                remote(osend.at[0], orecv.at[slot], o_send.at[0], o_recv.at[slot], (b, sib)).wait_recv()
    low2 = lax.broadcasted_iota(jnp.int32, (td // 2, LANES), 1) < HD
    for p in range(heads * nh // 2):
        even, odd = orecv[2 * p].astype(F32), orecv[2 * p + 1].astype(F32)
        c = pl.ds(p * LANES, LANES)
        mixed[pl.ds(0, td // 2), c] = jnp.where(low2, even, pltpu.roll(odd, HD, 1)).astype(BF16)
        mixed[pl.ds(td // 2, td // 2), c] = jnp.where(low2, pltpu.roll(even, HD, 1), odd).astype(BF16)

    unit = min(td, BS)
    width = 256
    for t in range(out_ref.shape[1] // width):
        c = pl.ds(t * width, width)
        y = jnp.dot(mixed[...], wfull[:, c], preferred_element_type=F32)
        for u in range(td // unit):
            image = img_ref[(b * tok + j * td + u * unit) // BS]
            gate = jnp.zeros((1, width), F32)
            for m in range(images):
                gate = jnp.where(image == m, gate_ref[pl.ds(m, 1), c], gate)
            rows = pl.ds(u * unit, unit)
            part = y[u * unit:(u + 1) * unit]
            out_ref[rows, c] = (resv[rows, c].astype(F32) + gate * part).astype(BF16)

    for copy in sent:
        copy.wait_send()


QROWS = 128
VROWS = 80


def split_kernel(
    n, nh, q_ref, k_ref, v_ref, tk_ref, tv_ref, img_ref, gate_ref, res_ref, w_ref, out_ref,
    qin, kin, vin, tkin, tvin, qt, vt, ks, kr, qa, kaug, va, traw, sb, mb, osend, lsend, orecv, lrecv,
    mixed, wfull, resv,
    q_send, q_recv, k_send, k_recv, v_send, v_recv, wx_send, ws_send, w_recv, o_send, o_recv, e_send, e_recv, l_sem,
):
    tok, cols = q_ref.shape
    heads = cols // HD
    groups = n // heads
    half = tok // 2
    images = gate_ref.shape[0]
    wrows = w_ref.shape[0]
    td = res_ref.shape[0]
    texts = tk_ref.shape[0]
    share = -(-texts // groups)
    keys = heads * tok
    allk = kaug.shape[0]
    tpad = allk - keys
    per = tok // BS
    b = lax.axis_index("blk")
    j = lax.axis_index("head")
    z, r = b % heads, b // heads
    side, core = j // 2, j % 2

    barrier = pltpu.get_barrier_semaphore()
    count = 0
    for k in range(groups):
        for i in range(heads):
            if i or k:
                to = (lax.rem(r + k, groups) * heads + partner(z, i), j)
                pl.semaphore_signal(barrier, inc=1, device_id=to, device_id_type=MESH)
                count += 1
    for k in range(1, nh):
        pl.semaphore_signal(barrier, inc=1, device_id=(b, lax.rem(j + k, nh)), device_id_type=MESH)
        count += 1

    local = []
    for s, (src, dst) in enumerate(
        ((v_ref, vin), (q_ref, qin), (k_ref, kin), (tk_ref, tkin), (tv_ref, tvin),
         (w_ref, wfull.at[pl.ds(pl.multiple_of(j * wrows, wrows), wrows)]), (res_ref, resv))
    ):
        copy = pltpu.make_async_copy(src, dst, l_sem.at[s])
        copy.start()
        local.append(copy)

    def remote(src, dst, ss, rs, to):
        return pltpu.make_async_remote_copy(
            src_ref=src, dst_ref=dst, send_sem=ss, recv_sem=rs, device_id=to, device_id_type=MESH
        )

    sent = []

    def go(copy):
        copy.start()
        sent.append(copy)

    local[0].wait()
    vt[...] = jnp.transpose(vin[...])
    local[2].wait()
    for h in range(heads):
        c = slice(h * HD, (h + 1) * HD)
        kh = kin[:, c]
        ks[h] = jnp.concatenate([kh[:half], kh[half:]], axis=1)
    local[1].wait()
    qt[...] = jnp.transpose(qin[...]) * BF16(HD ** -0.5)

    pl.semaphore_wait(barrier, count)

    def hrows(h):
        return pl.ds(pl.multiple_of(h * HD, HD), HD)

    for i in range(1, heads):
        other = partner(z, i)
        to = (r * heads + other, j)
        go(remote(ks.at[other], kr.at[i], k_send.at[i], k_recv.at[i], to))
        go(remote(vt.at[hrows(other)], va.at[pl.ds(0, HD), pl.ds(i * tok, tok)], v_send.at[i], v_recv.at[i], to))

    def send_q(k, i):
        other = partner(z, i)
        pos = (groups - k) % groups * heads + i
        go(remote(qt.at[hrows(other)], qa.at[pos, pl.ds(0, HD)], q_send.at[pos], q_recv.at[pos],
                  (lax.rem(r + k, groups) * heads + other, j)))

    for k in range(1, groups):
        for i in range(heads):
            send_q(k, i)
    for i in range(1, heads):
        send_q(0, i)

    def wrow(owner):
        return wfull.at[pl.ds(pl.multiple_of(owner * wrows, wrows), wrows)]

    sib = side * 2 + 1 - core
    go(remote(w_ref, wrow(j), ws_send.at[0], w_recv.at[j], (b, sib)))
    for k in range(1, nh // 2):
        to = lax.rem(side + k, nh // 2) * 2 + core
        go(remote(w_ref, wrow(j), wx_send.at[k], w_recv.at[j], (b, to)))

    lane = lax.broadcasted_iota(jnp.int32, (16, LANES), 1)
    low_f = (lane < HD).astype(F32)
    low = low_f.astype(BF16)[:1]

    def onehot(image):
        return jnp.where(lane == HD + image, 1.0, 0.0).astype(BF16)[:1]

    srow = lax.broadcasted_iota(jnp.int32, (QROWS - HD, BS), 0)
    for pos in range(n):
        first = (lax.rem(r + pos // heads, groups) * heads + partner(z, pos % heads)) * per
        for p in range(per):
            mask = jnp.where(srow == img_ref[first + p], 0.0, NEG).astype(BF16)
            qa[pos, pl.ds(HD, QROWS - HD), pl.ds(p * BS, BS)] = mask
    qa[0, pl.ds(0, HD), :] = qt[hrows(z), :]
    va[pl.ds(0, HD), pl.ds(0, tok)] = vt[hrows(z), :]
    va[pl.ds(HD, VROWS - HD), :] = jnp.ones((VROWS - HD, allk), BF16)

    local[3].wait()
    local[4].wait()
    traw[...] = jnp.zeros_like(traw)
    for h in range(heads):
        c = slice(h * HD, (h + 1) * HD)

        @pl.when(z == h)
        def _():
            traw[pl.ds(0, texts), :] = jnp.concatenate([tkin[:, c], tvin[:, c]], axis=1).astype(F32)

    span = -(-tpad // LANES) * LANES
    raw = traw[pl.ds(r * share, span), :]
    trow = lax.broadcasted_iota(jnp.int32, raw.shape, 0)
    tlane = lax.broadcasted_iota(jnp.int32, raw.shape, 1)
    timg = jnp.zeros_like(trow)
    for i in range(1, images + 1):
        timg += (trow + r * share >= i * TEXT).astype(jnp.int32)
    timg = jnp.where(trow < share, timg, images)
    taug = jnp.where(tlane < HD, raw, jnp.where(tlane == HD + timg, 1.0, 0.0)).astype(BF16)
    kaug[pl.ds(keys, tpad), :] = taug[:tpad]
    va[pl.ds(0, HD), pl.ds(keys, tpad)] = jnp.transpose(raw)[HD:, :tpad].astype(BF16)

    def load_k(i):
        first = (r * heads + partner(z, i)) * per
        for p in range(per):
            at = (p * BS) % half
            x = ks[z, pl.ds(at, BS), :] if i == 0 else kr[i, pl.ds(at, BS), :]
            if p * BS >= half:
                x = pltpu.roll(x.astype(F32), HD, 1).astype(BF16)
            kaug[pl.ds(i * tok + p * BS, BS), :] = x * low + onehot(img_ref[first + p])

    load_k(0)
    for i in range(1, heads):
        remote(ks.at[0], kr.at[i], k_send.at[i], k_recv.at[i], (b, sib)).wait_recv()
        load_k(i)
    for i in range(1, heads):
        remote(vt.at[pl.ds(0, HD)], va.at[pl.ds(0, HD), pl.ds(i * tok, tok)], v_send.at[i], v_recv.at[i],
               (b, sib)).wait_recv()

    order = [0] + list(range(heads, n)) + list(range(1, heads))

    def arrive(pos):
        if pos:
            remote(qt.at[pl.ds(0, HD)], qa.at[pos, pl.ds(0, HD)], q_send.at[pos], q_recv.at[pos],
                   (b, sib)).wait_recv()

    def scores(pos, slot):
        s = jnp.dot(kaug[...], qa[pos], preferred_element_type=F32)
        sb[slot] = s
        mb[slot] = jnp.broadcast_to(jnp.max(s, axis=0, keepdims=True), mb.shape[1:])

    def attend(pos, slot):
        top = mb[slot][:1]
        p = jnp.exp(sb[slot] - top).astype(BF16)
        o = jnp.dot(va[...], p, preferred_element_type=F32)
        den = o[HD:HD + 1]
        y = (o[:HD] / den).astype(BF16)
        level = top + jnp.log(den)
        for d in range(nh):
            osend[pos * nh + d] = y[:, d * td:(d + 1) * td]
            lsend[pos * nh + d] = level[:, d * td:(d + 1) * td]

    mine = (j * heads + z) * groups + r

    def give(pos, k):
        dest = lax.rem(j + k, nh)
        to = (lax.rem(r + pos // heads, groups) * heads + partner(z, pos % heads), dest)
        if pos == 0 and k == 0:
            orecv[mine] = osend[dest]
            lrecv[mine] = lsend[dest]
        else:
            at = pos * nh + dest
            go(remote(osend.at[at], orecv.at[mine], o_send.at[pos * nh + k], o_recv.at[mine], to))
            go(remote(lsend.at[at], lrecv.at[mine], e_send.at[pos * nh + k], e_recv.at[mine], to))

    def relay_w():
        for k in range(1, nh // 2):
            owner = lax.rem(side + nh // 2 - k, nh // 2) * 2 + core
            remote(w_ref, wrow(owner), ws_send.at[k], w_recv.at[owner], (b, sib)).wait_recv()
            go(remote(wrow(owner), wrow(owner), ws_send.at[k], w_recv.at[owner], (b, sib)))

    arrive(order[0])
    scores(order[0], 0)
    for t in range(n):
        pos = order[t]
        if t + 1 < n:
            arrive(order[t + 1])
            scores(order[t + 1], (t + 1) % 2)
        attend(pos, t % 2)
        for k in range(nh):
            give(pos, k)
    relay_w()

    local[5].wait()
    local[6].wait()
    for k in range(groups):
        for i in range(heads):
            for d in range(nh):
                if i or k or d:
                    slot = (lax.rem(j + d, nh) * heads + partner(z, i)) * groups + lax.rem(r + k, groups)
                    remote(osend.at[0], orecv.at[slot], o_send.at[0], o_recv.at[slot], (b, sib)).wait_recv()
                    remote(lsend.at[0], lrecv.at[slot], e_send.at[0], e_recv.at[slot], (b, sib)).wait_recv()
    for h in range(heads * nh):
        levels = [lrecv[h * groups + g] for g in range(groups)]
        top = functools.reduce(jnp.maximum, levels)
        ws = [jnp.exp(x - top) for x in levels]
        total = functools.reduce(jnp.add, ws)
        parts = [orecv[h * groups + g].astype(F32) * (ws[g] / total) for g in range(groups)]
        mixed[pl.ds(h * HD, HD), :] = functools.reduce(jnp.add, parts).astype(BF16)
    for k in range(nh // 2):
        owner = lax.rem(side + nh // 2 - k, nh // 2) * 2 + 1 - core
        remote(w_ref, wrow(owner), ws_send.at[k], w_recv.at[owner], (b, sib)).wait_recv()

    attended = jnp.transpose(mixed[...])
    unit = min(td, BS)
    width = 256
    for t in range(out_ref.shape[1] // width):
        c = pl.ds(t * width, width)
        y = jnp.dot(attended, wfull[:, c], preferred_element_type=F32)
        for u in range(td // unit):
            image = img_ref[(b * tok + j * td + u * unit) // BS]
            gate = jnp.zeros((1, width), F32)
            for m in range(images):
                gate = jnp.where(image == m, gate_ref[pl.ds(m, 1), c], gate)
            rows = pl.ds(u * unit, unit)
            part = y[u * unit:(u + 1) * unit]
            out_ref[rows, c] = (resv[rows, c].astype(F32) + gate * part).astype(BF16)

    for copy in sent:
        copy.wait_send()


def split_call(n, nh, *args):
    q, k, v, tk, tv, block_image, gate, res, w = args
    tok, cols = q.shape
    heads = cols // HD
    groups = n // heads
    td = res.shape[0]
    share = -(-tk.shape[0] // groups)
    tpad = -(-share // 16) * 16
    span = -(-tpad // LANES) * LANES
    keys = heads * tok + tpad
    vm = pl.BlockSpec(memory_space=pltpu.VMEM)
    anyw = pl.BlockSpec(memory_space=pl.ANY)
    dma = pltpu.SemaphoreType.DMA
    return pl.pallas_call(
        functools.partial(split_kernel, n, nh),
        out_shape=jax.ShapeDtypeStruct(res.shape, BF16),
        in_specs=[anyw] * 5 + [pl.BlockSpec(memory_space=pltpu.SMEM), vm, anyw, anyw],
        out_specs=vm,
        scratch_shapes=[
            pltpu.VMEM(q.shape, BF16), pltpu.VMEM(k.shape, BF16), pltpu.VMEM(v.shape, BF16),
            pltpu.VMEM(tk.shape, BF16), pltpu.VMEM(tv.shape, BF16),
            pltpu.VMEM((cols, tok), BF16), pltpu.VMEM((cols, tok), BF16),
            pltpu.VMEM((heads, tok // 2, LANES), BF16), pltpu.VMEM((heads, tok // 2, LANES), BF16),
            pltpu.VMEM((n, QROWS, tok), BF16),
            pltpu.VMEM((keys, LANES), BF16),
            pltpu.VMEM((VROWS, keys), BF16),
            pltpu.VMEM(((groups - 1) * share + max(span, tk.shape[0]) + 8, LANES), F32),
            pltpu.VMEM((2, keys, tok), F32),
            pltpu.VMEM((2, 8, tok), F32),
            pltpu.VMEM((n * nh, HD, td), BF16),
            pltpu.VMEM((n * nh, 1, td), F32),
            pltpu.VMEM((n * nh, HD, td), BF16),
            pltpu.VMEM((n * nh, 1, td), F32),
            pltpu.VMEM((heads * nh * HD, td), BF16),
            pltpu.VMEM((w.shape[0] * nh, w.shape[1]), BF16),
            pltpu.VMEM(res.shape, BF16),
            dma((n,)), dma((n,)), dma((heads,)), dma((heads,)), dma((heads,)), dma((heads,)),
            dma((nh,)), dma((nh,)), dma((nh,)),
            dma((n * nh,)), dma((n * nh,)), dma((n * nh,)), dma((n * nh,)), dma((7,)),
        ],
        compiler_params=pltpu.CompilerParams(
            collective_id=0, has_side_effects=True, vmem_limit_bytes=60 * 1024 * 1024
        ),
    )(*args)


def solution(mesh):
    n, nh = mesh.shape["blk"], mesh.shape["head"]

    def on_device(q, k, v, tk, tv, block_image, gate, res, w):
        tok, cols = q.shape
        heads = cols // HD
        groups = n // heads
        td = res.shape[0]
        rows = heads * tok
        if groups > 1 and groups <= 4 and td % LANES == 0 and tok % (2 * BS) == 0:
            return split_call(n, nh, q, k, v, tk, tv, block_image, gate, res, w)
        upad = -(-tk.shape[0] // LANES) * LANES
        vm = pl.BlockSpec(memory_space=pltpu.VMEM)
        anyw = pl.BlockSpec(memory_space=pl.ANY)
        dma = pltpu.SemaphoreType.DMA
        return pl.pallas_call(
            functools.partial(kernel, n, nh),
            out_shape=jax.ShapeDtypeStruct(res.shape, BF16),
            in_specs=[vm, vm, vm, vm, vm, pl.BlockSpec(memory_space=pltpu.SMEM), vm, anyw, anyw],
            out_specs=vm,
            scratch_shapes=[
                pltpu.VMEM((heads, tok // 2, LANES), BF16),
                pltpu.VMEM((heads, tok, LANES), BF16),
                pltpu.VMEM((heads, tok // 2, LANES), BF16),
                pltpu.VMEM((n, tok, LANES), BF16),
                pltpu.VMEM((upad, LANES), F32),
                pltpu.VMEM((rows, LANES), BF16),
                pltpu.VMEM((n * tok, LANES), BF16),
                pltpu.VMEM((n * tok, LANES), BF16),
                pltpu.VMEM((upad, LANES), BF16),
                pltpu.VMEM((upad, LANES), BF16),
                pltpu.VMEM((rows, LANES), F32),
                pltpu.VMEM((rows, LANES), F32),
                pltpu.VMEM((heads * nh, td // 2, LANES), BF16),
                pltpu.VMEM((heads * nh, td // 2, LANES), BF16),
                pltpu.VMEM((td, heads * nh * HD), BF16),
                pltpu.VMEM((w.shape[0] * nh, w.shape[1]), BF16),
                pltpu.VMEM(res.shape, BF16),
                dma((heads,)), dma((heads,)), dma((n,)), dma((n,)),
                dma((nh,)), dma((nh,)), dma((nh,)), dma((heads * nh,)), dma((heads * nh,)), dma((2,)),
            ],
            compiler_params=pltpu.CompilerParams(
                collective_id=0, has_side_effects=True, vmem_limit_bytes=60 * 1024 * 1024
            ),
        )(q, k, v, tk, tv, block_image, gate, res, w)

    placed = (
        P("blk", "head"), P("blk", "head"), P("blk", "head"), P(None, "head"), P(None, "head"),
        P(), P(), P(("blk", "head"), None), P("head", None),
    )
    return jax.shard_map(
        on_device, mesh=mesh, in_specs=placed, out_specs=P(("blk", "head"), None), check_vma=False
    )
```

```python
import functools

import jax
import jax.numpy as jnp
from jax import lax
from jax.experimental import pallas as pl
from jax.experimental.pallas import tpu as pltpu
from jax.sharding import PartitionSpec as P

HD = 64
TEXT = 154
BS = 128
NEG = -1e30
LANES = 128
QTILE = 512
KEYS = 1024
MESH = pl.DeviceIdType.MESH
F32 = jnp.float32
BF16 = jnp.bfloat16


def partner(z, i):
    out, bit = z, 1
    while bit <= i:
        if i & bit:
            out = out + bit - 2 * bit * ((out // bit) % 2)
        bit *= 2
    return out


def kernel(
    n, nh, q_ref, k_ref, v_ref, tk_ref, tv_ref, img_ref, gate_ref, res_ref, w_ref, out_ref,
    qs, kvs, qr, kvr, traw, qaug, kaug, kval, taug, tval, best, accum, osend, orecv, mixed, wfull, resv,
    q_send, q_recv, kv_send, kv_recv, wx_send, ws_send, w_recv, o_send, o_recv, l_sem,
):
    tok, cols = q_ref.shape
    heads = cols // HD
    groups = n // heads
    half = tok // 2
    images = gate_ref.shape[0]
    wrows = w_ref.shape[0]
    td = res_ref.shape[0]
    texts = tk_ref.shape[0]
    per = tok // BS
    b = lax.axis_index("blk")
    j = lax.axis_index("head")
    z, r = b % heads, b // heads
    side, core = j // 2, j % 2

    barrier = pltpu.get_barrier_semaphore()
    count = 0
    for i in range(heads):
        for k in range(nh):
            if i or k:
                to = (r * heads + partner(z, i), lax.rem(j + k, nh))
                pl.semaphore_signal(barrier, inc=1, device_id=to, device_id_type=MESH)
                count += 1
    for k in range(1, groups):
        for i in range(heads):
            to = (lax.rem(r + k, groups) * heads + partner(z, i), j)
            pl.semaphore_signal(barrier, inc=1, device_id=to, device_id_type=MESH)
            count += 1

    w_here = pltpu.make_async_copy(w_ref, wfull.at[pl.ds(pl.multiple_of(j * wrows, wrows), wrows)], l_sem.at[0])
    w_here.start()
    res_here = pltpu.make_async_copy(res_ref, resv, l_sem.at[1])
    res_here.start()

    for h in range(heads):
        c = slice(h * HD, (h + 1) * HD)
        q = q_ref[:, c] * BF16(HD ** -0.5)
        qs[h] = jnp.concatenate([q[:half], q[half:]], axis=1)
        kvs[h] = jnp.concatenate([k_ref[:, c], v_ref[:, c]], axis=1)

    pl.semaphore_wait(barrier, count)

    def remote(src, dst, ss, rs, to):
        return pltpu.make_async_remote_copy(
            src_ref=src, dst_ref=dst, send_sem=ss, recv_sem=rs, device_id=to, device_id_type=MESH
        )

    sent = []

    def go(copy):
        copy.start()
        sent.append(copy)

    def wrow(owner):
        return wfull.at[pl.ds(pl.multiple_of(owner * wrows, wrows), wrows)]

    def send_kv(i, k):
        other = partner(z, i)
        pos = (groups - k) % groups * heads + i
        go(remote(kvs.at[other], kvr.at[pos], kv_send.at[pos], kv_recv.at[pos],
                  (lax.rem(r + k, groups) * heads + other, j)))

    for i in range(1, heads):
        other = partner(z, i)
        go(remote(qs.at[other], qr.at[i], q_send.at[i], q_recv.at[i], (r * heads + other, j)))
    for i in range(1, heads):
        send_kv(i, 0)
    for i in range(heads):
        for k in range(1, groups):
            send_kv(i, k)
    sib = side * 2 + 1 - core
    go(remote(w_ref, wrow(j), ws_send.at[0], w_recv.at[j], (b, sib)))
    for k in range(1, nh // 2):
        to = lax.rem(side + k, nh // 2) * 2 + core
        go(remote(w_ref, wrow(j), wx_send.at[k], w_recv.at[j], (b, to)))

    lane = lax.broadcasted_iota(jnp.int32, (16, LANES), 1)
    low_f = (lane < HD).astype(F32)
    low = low_f.astype(BF16)[:1]
    high = (1.0 - low_f).astype(BF16)[:1]

    def onehot(image):
        return jnp.where(lane == HD + image, 1.0, 0.0).astype(BF16)[:1]

    def others(image):
        return jnp.where((lane < HD) | (lane == HD + image), 0.0, NEG).astype(BF16)[:1]

    traw[...] = jnp.zeros_like(traw)
    for h in range(heads):
        c = slice(h * HD, (h + 1) * HD)

        @pl.when(z == h)
        def _():
            traw[pl.ds(0, texts), :] = jnp.concatenate([tk_ref[:, c], tv_ref[:, c]], axis=1).astype(F32)

    trow = lax.broadcasted_iota(jnp.int32, traw.shape, 0)
    tlane = lax.broadcasted_iota(jnp.int32, traw.shape, 1)
    timg = jnp.zeros_like(trow)
    for i in range(1, images + 1):
        timg += (trow >= i * TEXT).astype(jnp.int32)
    raw = traw[...]
    taug[...] = jnp.where(tlane < HD, raw, jnp.where(tlane == HD + timg, 1.0, 0.0)).astype(BF16)
    tval[...] = jnp.where(tlane < HD, 1.0, raw).astype(BF16)

    def load_q(i):
        src = qs.at[z] if i == 0 else qr.at[i]
        first = (r * heads + partner(z, i)) * per
        for p in range(per):
            at = (p * BS) % half
            x = src[pl.ds(at, BS), :]
            if p * BS >= half:
                x = pltpu.roll(x.astype(F32), HD, 1).astype(BF16)
            qaug[pl.ds(i * tok + p * BS, BS), :] = x * low + others(img_ref[first + p])

    def load_kv(pos):
        first = (lax.rem(r + pos // heads, groups) * heads + partner(z, pos % heads)) * per
        for p in range(per):
            x = kvr[pos, pl.ds(p * BS, BS), :]
            rows = pl.ds(pos * tok + p * BS, BS)
            kaug[rows, :] = x * low + onehot(img_ref[first + p])
            kval[rows, :] = x * high + low

    def absorb(keys, vals, start, count, fresh):
        def body(t, carry):
            rows = pl.ds(pl.multiple_of(start + t * QTILE, QTILE), QTILE)
            s = lax.dot_general(qaug[rows, :], keys(), (((1,), (1,)), ((), ())), preferred_element_type=F32)
            top = jnp.broadcast_to(jnp.max(s, axis=1, keepdims=True), (QTILE, LANES))
            if not fresh:
                old = best[rows, :]
                top = jnp.maximum(old, top)
            wide = jnp.concatenate([top] * (s.shape[1] // LANES), axis=1)
            p = jnp.exp(s - wide).astype(BF16)
            add = jnp.dot(p, vals(), preferred_element_type=F32)
            if fresh:
                accum[rows, :] = add
            else:
                accum[rows, :] = accum[rows, :] * jnp.exp(old - top) + add
            best[rows, :] = top
            return carry

        lax.fori_loop(0, count // QTILE, body, 0, unroll=1)

    kvr[0] = kvs[z]
    for i in range(heads):
        if i:
            remote(qs.at[0], qr.at[i], q_send.at[i], q_recv.at[i], (b, sib)).wait_recv()
        load_q(i)
        absorb(lambda: taug[...], lambda: tval[...], i * tok, tok, True)

    join = max(1, min(heads, KEYS // tok))

    def arrive(pos):
        remote(kvs.at[0], kvr.at[pos], kv_send.at[0], kv_recv.at[pos], (b, sib)).wait_recv()

    def relay_w():
        for k in range(1, nh // 2):
            owner = lax.rem(side + nh // 2 - k, nh // 2) * 2 + core
            remote(w_ref, wrow(owner), ws_send.at[k], w_recv.at[owner], (b, sib)).wait_recv()
            go(remote(wrow(owner), wrow(owner), ws_send.at[k], w_recv.at[owner], (b, sib)))

    def finish(i):
        low2 = lax.broadcasted_iota(jnp.int32, (td // 2, LANES), 1) < HD
        to_blk = r * heads + partner(z, i)
        slot = j * heads + z
        for k in range(nh):
            dest = lax.rem(j + k, nh)
            base = pl.multiple_of(i * tok + dest * td, td)
            one = accum[pl.ds(base, td // 2), :]
            two = accum[pl.ds(base + td // 2, td // 2), :]
            one_r, two_r = pltpu.roll(one, HD, 1), pltpu.roll(two, HD, 1)
            y = (jnp.where(low2, one_r, two) / jnp.where(low2, one, two_r)).astype(BF16)
            if i == 0 and k == 0:
                orecv[slot] = y
            else:
                osend[i * nh + k] = y
                go(remote(osend.at[i * nh + k], orecv.at[slot], o_send.at[i * nh + k], o_recv.at[slot],
                          (to_blk, dest)))

    for g in range(0, n, join):
        for pos in range(g, g + join):
            if pos:
                arrive(pos)
            load_kv(pos)
        at = pl.ds(g * tok, join * tok)
        args = (lambda: kaug[at, :], lambda: kval[at, :])
        if g + join == n:
            relay_w()
            for s in reversed(range(heads)):
                absorb(*args, s * tok, tok, False)
                finish(s)
        else:
            absorb(*args, 0, heads * tok, False)

    w_here.wait()
    res_here.wait()
    for k in range(nh // 2):
        owner = lax.rem(side + nh // 2 - k, nh // 2) * 2 + 1 - core
        remote(w_ref, wrow(owner), ws_send.at[k], w_recv.at[owner], (b, sib)).wait_recv()
    for i in range(heads):
        for k in range(nh):
            if i or k:
                slot = lax.rem(j + k, nh) * heads + partner(z, i)
                remote(osend.at[0], orecv.at[slot], o_send.at[0], o_recv.at[slot], (b, sib)).wait_recv()
    low2 = lax.broadcasted_iota(jnp.int32, (td // 2, LANES), 1) < HD
    for p in range(heads * nh // 2):
        even, odd = orecv[2 * p].astype(F32), orecv[2 * p + 1].astype(F32)
        c = pl.ds(p * LANES, LANES)
        mixed[pl.ds(0, td // 2), c] = jnp.where(low2, even, pltpu.roll(odd, HD, 1)).astype(BF16)
        mixed[pl.ds(td // 2, td // 2), c] = jnp.where(low2, pltpu.roll(even, HD, 1), odd).astype(BF16)

    unit = min(td, BS)
    width = 256
    for t in range(out_ref.shape[1] // width):
        c = pl.ds(t * width, width)
        y = jnp.dot(mixed[...], wfull[:, c], preferred_element_type=F32)
        for u in range(td // unit):
            image = img_ref[(b * tok + j * td + u * unit) // BS]
            gate = jnp.zeros((1, width), F32)
            for m in range(images):
                gate = jnp.where(image == m, gate_ref[pl.ds(m, 1), c], gate)
            rows = pl.ds(u * unit, unit)
            part = y[u * unit:(u + 1) * unit]
            out_ref[rows, c] = (resv[rows, c].astype(F32) + gate * part).astype(BF16)

    for copy in sent:
        copy.wait_send()


QROWS = 128
VROWS = 80


def split_kernel(
    n, nh, q_ref, k_ref, v_ref, tk_ref, tv_ref, img_in, gate_in, res_ref, w_ref, out_ref,
    qin, kin, vin, tkin, tvin, img_ref, gate_ref, qt, vt, ks, kr, qa, kaug, va, traw, sb, mb, osend, lsend, orecv, lrecv,
    mixed, wfull, resv,
    q_send, q_recv, k_send, k_recv, v_send, v_recv, wx_send, ws_send, w_recv, o_send, o_recv, e_send, e_recv, l_sem,
):
    tok, cols = q_ref.shape
    heads = cols // HD
    groups = n // heads
    half = tok // 2
    images = gate_ref.shape[0]
    wrows = w_ref.shape[0]
    td = res_ref.shape[0]
    texts = tk_ref.shape[0]
    share = -(-texts // groups)
    keys = heads * tok
    allk = kaug.shape[0]
    tpad = allk - keys
    per = tok // BS
    b = lax.axis_index("blk")
    j = lax.axis_index("head")
    z, r = b % heads, b // heads
    side, core = j // 2, j % 2

    barrier = pltpu.get_barrier_semaphore()
    count = 0
    for k in range(groups):
        for i in range(heads):
            if i or k:
                to = (lax.rem(r + k, groups) * heads + partner(z, i), j)
                pl.semaphore_signal(barrier, inc=1, device_id=to, device_id_type=MESH)
                count += 1
    for k in range(1, nh):
        pl.semaphore_signal(barrier, inc=1, device_id=(b, lax.rem(j + k, nh)), device_id_type=MESH)
        count += 1

    local = []
    for s, (src, dst) in enumerate(
        ((v_ref, vin), (q_ref, qin), (k_ref, kin), (tk_ref, tkin), (tv_ref, tvin),
         (img_in, img_ref), (gate_in, gate_ref),
         (w_ref, wfull.at[pl.ds(pl.multiple_of(j * wrows, wrows), wrows)]), (res_ref, resv))
    ):
        copy = pltpu.make_async_copy(src, dst, l_sem.at[s])
        copy.start()
        local.append(copy)

    def remote(src, dst, ss, rs, to):
        return pltpu.make_async_remote_copy(
            src_ref=src, dst_ref=dst, send_sem=ss, recv_sem=rs, device_id=to, device_id_type=MESH
        )

    def go(copy):
        copy.start()

    local[0].wait()
    vt[...] = jnp.transpose(vin[...])
    local[2].wait()
    for h in range(heads):
        c = slice(h * HD, (h + 1) * HD)
        kh = kin[:, c]
        ks[h] = jnp.concatenate([kh[:half], kh[half:]], axis=1)
    local[1].wait()
    qt[...] = jnp.transpose(qin[...]) * BF16(HD ** -0.5)

    pl.semaphore_wait(barrier, count)

    def hrows(h):
        return pl.ds(pl.multiple_of(h * HD, HD), HD)

    def send_k(i):
        other = partner(z, i)
        go(remote(ks.at[other], kr.at[i], k_send, k_recv.at[i], (r * heads + other, j)))

    def send_v(i):
        other = partner(z, i)
        go(remote(vt.at[hrows(other)], va.at[pl.ds(0, HD), pl.ds(i * tok, tok)], v_send, v_recv,
                  (r * heads + other, j)))

    flip = (z * 2 // heads + r) % 2 * (heads // 2)
    near = lax.rem(z + flip, heads)

    def send_q(k, i):
        at = partner(flip, i) if k else i
        other = partner(near, i) if k else partner(z, i)
        pos = (groups - k) % groups * heads + at
        go(remote(qt.at[hrows(other)], qa.at[pos, pl.ds(0, HD)], q_send, q_recv.at[pos],
                  (lax.rem(r + k, groups) * heads + other, j)))

    close = (z * 2 // heads + r) % 2

    def send_cross(part):
        for k in range(1, groups):
            for i in part:
                send_q(k, i)

    def send_within(part):
        for i in part:
            send_q(0, i)

    def wrow(owner):
        return wfull.at[pl.ds(pl.multiple_of(owner * wrows, wrows), wrows)]

    sib = side * 2 + 1 - core
    go(remote(w_ref, wrow(j), ws_send, w_recv.at[j], (b, sib)))

    def arrived_w(owner):
        remote(w_ref, wrow(owner), ws_send, w_recv.at[owner], (b, sib)).wait_recv()

    def cross_w(src, owner):
        for k in range(1, nh // 2):
            to = lax.rem(side + k, nh // 2) * 2 + core
            go(remote(src, wrow(owner), wx_send, w_recv.at[owner], (b, to)))

    partners = list(range(heads // 2, heads)) + list(range(1, heads // 2))
    for i in partners:
        send_k(i)
    for i in partners:
        send_v(i)
    send_cross(range(heads // 2))
    send_within(range(1, heads // 2))

    @pl.when(close == 1)
    def _():
        send_within(range(heads // 2, heads))

    @pl.when(core == 1)
    def _():
        cross_w(w_ref, j)

    lane = lax.broadcasted_iota(jnp.int32, (16, LANES), 1)
    low_f = (lane < HD).astype(F32)
    low = low_f.astype(BF16)[:1]

    def onehot(image):
        return jnp.where(lane == HD + image, 1.0, 0.0).astype(BF16)[:1]

    local[5].wait()
    srow = lax.broadcasted_iota(jnp.int32, (QROWS - HD, BS), 0)
    for pos in range(n):
        first = (lax.rem(r + pos // heads, groups) * heads + partner(z, pos % heads)) * per
        for p in range(per):
            mask = jnp.where(srow == img_ref[first + p], 0.0, NEG).astype(BF16)
            qa[pos, pl.ds(HD, QROWS - HD), pl.ds(p * BS, BS)] = mask
    qa[0, pl.ds(0, HD), :] = qt[hrows(z), :]
    va[pl.ds(0, HD), pl.ds(0, tok)] = vt[hrows(z), :]
    va[pl.ds(HD, VROWS - HD), :] = jnp.ones((VROWS - HD, allk), BF16)

    local[3].wait()
    local[4].wait()
    traw[...] = jnp.zeros_like(traw)
    for h in range(heads):
        c = slice(h * HD, (h + 1) * HD)

        @pl.when(z == h)
        def _():
            traw[pl.ds(0, texts), :] = jnp.concatenate([tkin[:, c], tvin[:, c]], axis=1).astype(F32)

    span = -(-tpad // LANES) * LANES
    raw = traw[pl.ds(r * share, span), :]
    trow = lax.broadcasted_iota(jnp.int32, raw.shape, 0)
    tlane = lax.broadcasted_iota(jnp.int32, raw.shape, 1)
    timg = jnp.zeros_like(trow)
    for i in range(1, images + 1):
        timg += (trow + r * share >= i * TEXT).astype(jnp.int32)
    timg = jnp.where(trow < share, timg, images)
    taug = jnp.where(tlane < HD, raw, jnp.where(tlane == HD + timg, 1.0, 0.0)).astype(BF16)
    kaug[pl.ds(keys, tpad), :] = taug[:tpad]
    va[pl.ds(0, HD), pl.ds(keys, tpad)] = jnp.transpose(raw)[HD:, :tpad].astype(BF16)

    def load_k(i):
        first = (r * heads + partner(z, i)) * per
        for p in range(per):
            at = (p * BS) % half
            x = ks[z, pl.ds(at, BS), :] if i == 0 else kr[i, pl.ds(at, BS), :]
            if p * BS >= half:
                x = pltpu.roll(x.astype(F32), HD, 1).astype(BF16)
            kaug[pl.ds(i * tok + p * BS, BS), :] = x * low + onehot(img_ref[first + p])

    load_k(0)
    for i in partners:
        remote(ks.at[0], kr.at[i], k_send, k_recv.at[i], (b, sib)).wait_recv()
        load_k(i)
    send_cross(range(heads // 2, heads))

    @pl.when(close == 0)
    def _():
        send_within(range(heads // 2, heads))

    def blk(d, place):
        return lax.rem(r + d, groups) * heads + place

    own = [(i, blk(0, partner(z, i))) for i in range(heads)]
    cross = [
        (d * heads + partner(flip, i), blk(d, partner(near, i)))
        for d in range(1, groups) for i in range(heads)
    ]
    order = own[:1] + [
        tuple(close * u + (1 - close) * v for u, v in zip(one, two))
        for one, two in zip(cross + own[1:], own[1:] + cross[len(cross) // 2:] + cross[:len(cross) // 2])
    ]

    def arrive(pos):
        remote(qt.at[pl.ds(0, HD)], qa.at[pos, pl.ds(0, HD)], q_send, q_recv.at[pos], (b, sib)).wait_recv()

    def scores(pos, slot, low, width):
        c = pl.ds(low, width)
        s = jnp.dot(kaug[...], qa[pos, :, c], preferred_element_type=F32)
        sb[slot, :, c] = s
        mb[slot, :, c] = jnp.broadcast_to(jnp.max(s, axis=0, keepdims=True), (mb.shape[1], width))

    def attend(pos, slot, low, width):
        c = pl.ds(low, width)
        top = mb[slot, pl.ds(0, 1), c]
        p = jnp.exp(sb[slot, :, c] - top).astype(BF16)
        o = jnp.dot(va[...], p, preferred_element_type=F32)
        den = o[HD:HD + 1]
        y = (o[:HD] / den).astype(BF16)
        level = top + jnp.log(den)
        for d in range(width // td):
            osend[pos * nh + low // td + d] = y[:, d * td:(d + 1) * td]
            lsend[pos * nh + low // td + d] = level[:, d * td:(d + 1) * td]

    mine = (j * heads + z) * groups + r

    def give(pos, owner, dests):
        for dest in dests:
            at = pos * nh + dest
            go(remote(osend.at[at], orecv.at[mine], o_send, o_recv, (owner, dest)))
            go(remote(lsend.at[at], lrecv.at[mine], e_send, e_recv, (owner, dest)))

    def relay_w():
        @pl.when(core == 1)
        def _():
            for k in range(1, nh // 2):
                for c in range(2):
                    owner = lax.rem(side + k, nh // 2) * 2 + 1 - c
                    arrived_w(owner)
                    go(remote(wrow(owner), wrow(owner), ws_send, w_recv.at[owner], (b, sib)))

    scores(0, 0, 0, tok)
    rest = va.at[pl.ds(0, HD), pl.ds(tok, keys - tok)]
    remote(rest, rest, v_send, v_recv, (b, sib)).wait_recv()
    @pl.when(core == 1)
    def _():
        arrived_w(sib)
        cross_w(wrow(sib), sib)


    for t, (pos, owner) in enumerate(order):
        if t + 1 < n:
            arrive(order[t + 1][0])
            scores(order[t + 1][0], (t + 1) % 2, 0, tok)
        attend(pos, t % 2, 0, tok)
        if t == 0:
            orecv[mine] = osend[j]
            lrecv[mine] = lsend[j]
        turns = [(k + nh // 2) % nh for k in range(nh)]
        give(pos, owner, [lax.rem(j + k, nh) for k in turns if k or t])
    relay_w()

    local[6].wait()
    local[7].wait()
    local[8].wait()
    most = pl.ds(0, n * nh - 1)
    outs = remote(osend.at[most], orecv.at[most], o_send, o_recv, (b, sib))
    ends = remote(lsend.at[most], lrecv.at[most], e_send, e_recv, (b, sib))
    outs.wait_recv()
    ends.wait_recv()
    for h in range(heads * nh):
        levels = [lrecv[h * groups + g] for g in range(groups)]
        top = functools.reduce(jnp.maximum, levels)
        ws = [jnp.exp(x - top) for x in levels]
        total = functools.reduce(jnp.add, ws)
        parts = [orecv[h * groups + g].astype(F32) * (ws[g] / total) for g in range(groups)]
        mixed[pl.ds(h * HD, HD), :] = functools.reduce(jnp.add, parts).astype(BF16)
    @pl.when(core == 0)
    def _():
        arrived_w(sib)
        for k in range(1, nh // 2):
            for c in range(2):
                arrived_w(lax.rem(side + k, nh // 2) * 2 + c)

    attended = jnp.transpose(mixed[...])
    unit = min(td, BS)
    width = 256
    for t in range(out_ref.shape[1] // width):
        c = pl.ds(t * width, width)
        y = jnp.dot(attended, wfull[:, c], preferred_element_type=F32)
        for u in range(td // unit):
            image = img_ref[(b * tok + j * td + u * unit) // BS]
            gate = jnp.zeros((1, width), F32)
            for m in range(images):
                gate = jnp.where(image == m, gate_ref[pl.ds(m, 1), c], gate)
            rows = pl.ds(u * unit, unit)
            part = y[u * unit:(u + 1) * unit]
            out_ref[rows, c] = (resv[rows, c].astype(F32) + gate * part).astype(BF16)

    outs.wait_send()
    ends.wait_send()
    most = pl.ds(0, heads - 1)
    remote(ks.at[most], kr.at[most], k_send, k_recv.at[0], (b, sib)).wait_send()
    remote(rest, rest, v_send, v_recv, (b, sib)).wait_send()
    most = pl.ds(0, n - 1)
    part = qa.at[most, pl.ds(0, HD)]
    remote(part, part, q_send, q_recv.at[0], (b, sib)).wait_send()
    remote(w_ref, wrow(j), ws_send, w_recv.at[j], (b, sib)).wait_send()

    @pl.when(core == 1)
    def _():
        part = wfull.at[pl.ds(0, (nh - 2) * wrows)]
        remote(part, part, wx_send, w_recv.at[0], (b, sib)).wait_send()
        remote(part, part, ws_send, w_recv.at[0], (b, sib)).wait_send()


def split_call(n, nh, *args):
    q, k, v, tk, tv, block_image, gate, res, w = args
    tok, cols = q.shape
    heads = cols // HD
    groups = n // heads
    td = res.shape[0]
    share = -(-tk.shape[0] // groups)
    tpad = -(-share // 16) * 16
    span = -(-tpad // LANES) * LANES
    keys = heads * tok + tpad
    vm = pl.BlockSpec(memory_space=pltpu.VMEM)
    hbm = pl.BlockSpec(memory_space=pltpu.HBM)
    dma = pltpu.SemaphoreType.DMA
    return pl.pallas_call(
        functools.partial(split_kernel, n, nh),
        out_shape=pltpu.VMEM(res.shape, BF16),
        in_specs=[hbm] * 9,
        out_specs=vm,
        scratch_shapes=[
            pltpu.VMEM(q.shape, BF16), pltpu.VMEM(k.shape, BF16), pltpu.VMEM(v.shape, BF16),
            pltpu.VMEM(tk.shape, BF16), pltpu.VMEM(tv.shape, BF16),
            pltpu.SMEM(block_image.shape, jnp.int32), pltpu.VMEM(gate.shape, F32),
            pltpu.VMEM((cols, tok), BF16), pltpu.VMEM((cols, tok), BF16),
            pltpu.VMEM((heads, tok // 2, LANES), BF16), pltpu.VMEM((heads, tok // 2, LANES), BF16),
            pltpu.VMEM((n, QROWS, tok), BF16),
            pltpu.VMEM((keys, LANES), BF16),
            pltpu.VMEM((VROWS, keys), BF16),
            pltpu.VMEM(((groups - 1) * share + max(span, tk.shape[0]) + 8, LANES), F32),
            pltpu.VMEM((2, keys, tok), F32),
            pltpu.VMEM((2, 8, tok), F32),
            pltpu.VMEM((n * nh, HD, td), BF16),
            pltpu.VMEM((n * nh, 1, td), F32),
            pltpu.VMEM((n * nh, HD, td), BF16),
            pltpu.VMEM((n * nh, 1, td), F32),
            pltpu.VMEM((heads * nh * HD, td), BF16),
            pltpu.VMEM((w.shape[0] * nh, w.shape[1]), BF16),
            pltpu.VMEM(res.shape, BF16),
            dma, dma((n,)), dma, dma((heads,)), dma, dma,
            dma, dma, dma((nh,)), dma, dma, dma, dma, dma((9,)),
        ],
        compiler_params=pltpu.CompilerParams(
            collective_id=0, has_side_effects=True, vmem_limit_bytes=40 * 1024 * 1024
        ),
    )(*(pltpu.with_memory_space_constraint(x, pltpu.HBM) for x in args))


def solution(mesh):
    n, nh = mesh.shape["blk"], mesh.shape["head"]

    def on_device(q, k, v, tk, tv, block_image, gate, res, w):
        tok, cols = q.shape
        heads = cols // HD
        groups = n // heads
        td = res.shape[0]
        rows = heads * tok
        if 1 < groups <= 4 and heads > 1 and td % LANES == 0 and tok % (2 * BS) == 0:
            return split_call(n, nh, q, k, v, tk, tv, block_image, gate, res, w)
        upad = -(-tk.shape[0] // LANES) * LANES
        vm = pl.BlockSpec(memory_space=pltpu.VMEM)
        anyw = pl.BlockSpec(memory_space=pl.ANY)
        dma = pltpu.SemaphoreType.DMA
        return pl.pallas_call(
            functools.partial(kernel, n, nh),
            out_shape=jax.ShapeDtypeStruct(res.shape, BF16),
            in_specs=[vm, vm, vm, vm, vm, pl.BlockSpec(memory_space=pltpu.SMEM), vm, anyw, anyw],
            out_specs=vm,
            scratch_shapes=[
                pltpu.VMEM((heads, tok // 2, LANES), BF16),
                pltpu.VMEM((heads, tok, LANES), BF16),
                pltpu.VMEM((heads, tok // 2, LANES), BF16),
                pltpu.VMEM((n, tok, LANES), BF16),
                pltpu.VMEM((upad, LANES), F32),
                pltpu.VMEM((rows, LANES), BF16),
                pltpu.VMEM((n * tok, LANES), BF16),
                pltpu.VMEM((n * tok, LANES), BF16),
                pltpu.VMEM((upad, LANES), BF16),
                pltpu.VMEM((upad, LANES), BF16),
                pltpu.VMEM((rows, LANES), F32),
                pltpu.VMEM((rows, LANES), F32),
                pltpu.VMEM((heads * nh, td // 2, LANES), BF16),
                pltpu.VMEM((heads * nh, td // 2, LANES), BF16),
                pltpu.VMEM((td, heads * nh * HD), BF16),
                pltpu.VMEM((w.shape[0] * nh, w.shape[1]), BF16),
                pltpu.VMEM(res.shape, BF16),
                dma((heads,)), dma((heads,)), dma((n,)), dma((n,)),
                dma((nh,)), dma((nh,)), dma((nh,)), dma((heads * nh,)), dma((heads * nh,)), dma((2,)),
            ],
            compiler_params=pltpu.CompilerParams(
                collective_id=0, has_side_effects=True, vmem_limit_bytes=60 * 1024 * 1024
            ),
        )(q, k, v, tk, tv, block_image, gate, res, w)

    placed = (
        P("blk", "head"), P("blk", "head"), P("blk", "head"), P(None, "head"), P(None, "head"),
        P(), P(), P(("blk", "head"), None), P("head", None),
    )
    return jax.shard_map(
        on_device, mesh=mesh, in_specs=placed, out_specs=P(("blk", "head"), None), check_vma=False
    )
```

```python
import functools

import jax
import jax.numpy as jnp
from jax import lax
from jax.experimental import pallas as pl
from jax.experimental.pallas import tpu as pltpu
from jax.sharding import PartitionSpec as P

HD = 64
TEXT = 154
BS = 128
NEG = -1e30
LANES = 128
QTILE = 512
KEYS = 1024
MESH = pl.DeviceIdType.MESH
F32 = jnp.float32
BF16 = jnp.bfloat16


def partner(z, i):
    out, bit = z, 1
    while bit <= i:
        if i & bit:
            out = out + bit - 2 * bit * ((out // bit) % 2)
        bit *= 2
    return out


def kernel(
    n, nh, q_ref, k_ref, v_ref, tk_ref, tv_ref, img_ref, gate_ref, res_ref, w_ref, out_ref,
    qs, kvs, qr, kvr, traw, qaug, kaug, kval, taug, tval, best, accum, osend, orecv, mixed, wfull, resv,
    q_send, q_recv, kv_send, kv_recv, wx_send, ws_send, w_recv, o_send, o_recv, l_sem,
):
    tok, cols = q_ref.shape
    heads = cols // HD
    groups = n // heads
    half = tok // 2
    images = gate_ref.shape[0]
    wrows = w_ref.shape[0]
    td = res_ref.shape[0]
    texts = tk_ref.shape[0]
    per = tok // BS
    b = lax.axis_index("blk")
    j = lax.axis_index("head")
    z, r = b % heads, b // heads
    side, core = j // 2, j % 2

    barrier = pltpu.get_barrier_semaphore()
    count = 0
    for i in range(heads):
        for k in range(nh):
            if i or k:
                to = (r * heads + partner(z, i), lax.rem(j + k, nh))
                pl.semaphore_signal(barrier, inc=1, device_id=to, device_id_type=MESH)
                count += 1
    for k in range(1, groups):
        for i in range(heads):
            to = (lax.rem(r + k, groups) * heads + partner(z, i), j)
            pl.semaphore_signal(barrier, inc=1, device_id=to, device_id_type=MESH)
            count += 1

    w_here = pltpu.make_async_copy(w_ref, wfull.at[pl.ds(pl.multiple_of(j * wrows, wrows), wrows)], l_sem.at[0])
    w_here.start()
    res_here = pltpu.make_async_copy(res_ref, resv, l_sem.at[1])
    res_here.start()

    for h in range(heads):
        c = slice(h * HD, (h + 1) * HD)
        q = q_ref[:, c] * BF16(HD ** -0.5)
        qs[h] = jnp.concatenate([q[:half], q[half:]], axis=1)
        kvs[h] = jnp.concatenate([k_ref[:, c], v_ref[:, c]], axis=1)

    pl.semaphore_wait(barrier, count)

    def remote(src, dst, ss, rs, to):
        return pltpu.make_async_remote_copy(
            src_ref=src, dst_ref=dst, send_sem=ss, recv_sem=rs, device_id=to, device_id_type=MESH
        )

    sent = []

    def go(copy):
        copy.start()
        sent.append(copy)

    def wrow(owner):
        return wfull.at[pl.ds(pl.multiple_of(owner * wrows, wrows), wrows)]

    def send_kv(i, k):
        other = partner(z, i)
        pos = (groups - k) % groups * heads + i
        go(remote(kvs.at[other], kvr.at[pos], kv_send.at[pos], kv_recv.at[pos],
                  (lax.rem(r + k, groups) * heads + other, j)))

    for i in range(1, heads):
        other = partner(z, i)
        go(remote(qs.at[other], qr.at[i], q_send.at[i], q_recv.at[i], (r * heads + other, j)))
    for i in range(1, heads):
        send_kv(i, 0)
    for i in range(heads):
        for k in range(1, groups):
            send_kv(i, k)
    sib = side * 2 + 1 - core
    go(remote(w_ref, wrow(j), ws_send.at[0], w_recv.at[j], (b, sib)))
    for k in range(1, nh // 2):
        to = lax.rem(side + k, nh // 2) * 2 + core
        go(remote(w_ref, wrow(j), wx_send.at[k], w_recv.at[j], (b, to)))

    lane = lax.broadcasted_iota(jnp.int32, (16, LANES), 1)
    low_f = (lane < HD).astype(F32)
    low = low_f.astype(BF16)[:1]
    high = (1.0 - low_f).astype(BF16)[:1]

    def onehot(image):
        return jnp.where(lane == HD + image, 1.0, 0.0).astype(BF16)[:1]

    def others(image):
        return jnp.where((lane < HD) | (lane == HD + image), 0.0, NEG).astype(BF16)[:1]

    traw[...] = jnp.zeros_like(traw)
    for h in range(heads):
        c = slice(h * HD, (h + 1) * HD)

        @pl.when(z == h)
        def _():
            traw[pl.ds(0, texts), :] = jnp.concatenate([tk_ref[:, c], tv_ref[:, c]], axis=1).astype(F32)

    trow = lax.broadcasted_iota(jnp.int32, traw.shape, 0)
    tlane = lax.broadcasted_iota(jnp.int32, traw.shape, 1)
    timg = jnp.zeros_like(trow)
    for i in range(1, images + 1):
        timg += (trow >= i * TEXT).astype(jnp.int32)
    raw = traw[...]
    taug[...] = jnp.where(tlane < HD, raw, jnp.where(tlane == HD + timg, 1.0, 0.0)).astype(BF16)
    tval[...] = jnp.where(tlane < HD, 1.0, raw).astype(BF16)

    def load_q(i):
        src = qs.at[z] if i == 0 else qr.at[i]
        first = (r * heads + partner(z, i)) * per
        for p in range(per):
            at = (p * BS) % half
            x = src[pl.ds(at, BS), :]
            if p * BS >= half:
                x = pltpu.roll(x.astype(F32), HD, 1).astype(BF16)
            qaug[pl.ds(i * tok + p * BS, BS), :] = x * low + others(img_ref[first + p])

    def load_kv(pos):
        first = (lax.rem(r + pos // heads, groups) * heads + partner(z, pos % heads)) * per
        for p in range(per):
            x = kvr[pos, pl.ds(p * BS, BS), :]
            rows = pl.ds(pos * tok + p * BS, BS)
            kaug[rows, :] = x * low + onehot(img_ref[first + p])
            kval[rows, :] = x * high + low

    def absorb(keys, vals, start, count, fresh):
        def body(t, carry):
            rows = pl.ds(pl.multiple_of(start + t * QTILE, QTILE), QTILE)
            s = lax.dot_general(qaug[rows, :], keys(), (((1,), (1,)), ((), ())), preferred_element_type=F32)
            top = jnp.broadcast_to(jnp.max(s, axis=1, keepdims=True), (QTILE, LANES))
            if not fresh:
                old = best[rows, :]
                top = jnp.maximum(old, top)
            wide = jnp.concatenate([top] * (s.shape[1] // LANES), axis=1)
            p = jnp.exp(s - wide).astype(BF16)
            add = jnp.dot(p, vals(), preferred_element_type=F32)
            if fresh:
                accum[rows, :] = add
            else:
                accum[rows, :] = accum[rows, :] * jnp.exp(old - top) + add
            best[rows, :] = top
            return carry

        lax.fori_loop(0, count // QTILE, body, 0, unroll=1)

    kvr[0] = kvs[z]
    for i in range(heads):
        if i:
            remote(qs.at[0], qr.at[i], q_send.at[i], q_recv.at[i], (b, sib)).wait_recv()
        load_q(i)
        absorb(lambda: taug[...], lambda: tval[...], i * tok, tok, True)

    join = max(1, min(heads, KEYS // tok))

    def arrive(pos):
        remote(kvs.at[0], kvr.at[pos], kv_send.at[0], kv_recv.at[pos], (b, sib)).wait_recv()

    def relay_w():
        for k in range(1, nh // 2):
            owner = lax.rem(side + nh // 2 - k, nh // 2) * 2 + core
            remote(w_ref, wrow(owner), ws_send.at[k], w_recv.at[owner], (b, sib)).wait_recv()
            go(remote(wrow(owner), wrow(owner), ws_send.at[k], w_recv.at[owner], (b, sib)))

    def finish(i):
        low2 = lax.broadcasted_iota(jnp.int32, (td // 2, LANES), 1) < HD
        to_blk = r * heads + partner(z, i)
        slot = j * heads + z
        for k in range(nh):
            dest = lax.rem(j + k, nh)
            base = pl.multiple_of(i * tok + dest * td, td)
            one = accum[pl.ds(base, td // 2), :]
            two = accum[pl.ds(base + td // 2, td // 2), :]
            one_r, two_r = pltpu.roll(one, HD, 1), pltpu.roll(two, HD, 1)
            y = (jnp.where(low2, one_r, two) / jnp.where(low2, one, two_r)).astype(BF16)
            if i == 0 and k == 0:
                orecv[slot] = y
            else:
                osend[i * nh + k] = y
                go(remote(osend.at[i * nh + k], orecv.at[slot], o_send.at[i * nh + k], o_recv.at[slot],
                          (to_blk, dest)))

    for g in range(0, n, join):
        for pos in range(g, g + join):
            if pos:
                arrive(pos)
            load_kv(pos)
        at = pl.ds(g * tok, join * tok)
        args = (lambda: kaug[at, :], lambda: kval[at, :])
        if g + join == n:
            relay_w()
            for s in reversed(range(heads)):
                absorb(*args, s * tok, tok, False)
                finish(s)
        else:
            absorb(*args, 0, heads * tok, False)

    w_here.wait()
    res_here.wait()
    for k in range(nh // 2):
        owner = lax.rem(side + nh // 2 - k, nh // 2) * 2 + 1 - core
        remote(w_ref, wrow(owner), ws_send.at[k], w_recv.at[owner], (b, sib)).wait_recv()
    for i in range(heads):
        for k in range(nh):
            if i or k:
                slot = lax.rem(j + k, nh) * heads + partner(z, i)
                remote(osend.at[0], orecv.at[slot], o_send.at[0], o_recv.at[slot], (b, sib)).wait_recv()
    low2 = lax.broadcasted_iota(jnp.int32, (td // 2, LANES), 1) < HD
    for p in range(heads * nh // 2):
        even, odd = orecv[2 * p].astype(F32), orecv[2 * p + 1].astype(F32)
        c = pl.ds(p * LANES, LANES)
        mixed[pl.ds(0, td // 2), c] = jnp.where(low2, even, pltpu.roll(odd, HD, 1)).astype(BF16)
        mixed[pl.ds(td // 2, td // 2), c] = jnp.where(low2, pltpu.roll(even, HD, 1), odd).astype(BF16)

    unit = min(td, BS)
    width = 256
    for t in range(out_ref.shape[1] // width):
        c = pl.ds(t * width, width)
        y = jnp.dot(mixed[...], wfull[:, c], preferred_element_type=F32)
        for u in range(td // unit):
            image = img_ref[(b * tok + j * td + u * unit) // BS]
            gate = jnp.zeros((1, width), F32)
            for m in range(images):
                gate = jnp.where(image == m, gate_ref[pl.ds(m, 1), c], gate)
            rows = pl.ds(u * unit, unit)
            part = y[u * unit:(u + 1) * unit]
            out_ref[rows, c] = (resv[rows, c].astype(F32) + gate * part).astype(BF16)

    for copy in sent:
        copy.wait_send()


QROWS = 128
VROWS = 80


def split_kernel(
    n, nh, q_ref, k_ref, v_ref, tk_ref, tv_ref, img_in, gate_in, res_ref, w_ref, out_ref,
    qin, kin, vin, tkin, tvin, img_ref, gate_ref, qt, vt, ks, kr, qa, kaug, va, traw, sb, mb, osend, lsend, orecv, lrecv,
    mixed, wfull, resv,
    q_send, q_recv, k_send, k_recv, v_send, v_recv, wx_send, ws_send, w_recv, o_send, o_recv, e_send, e_recv, l_sem, told,
):
    tok, cols = q_ref.shape
    heads = cols // HD
    groups = n // heads
    half = tok // 2
    images = gate_ref.shape[0]
    wrows = w_ref.shape[0]
    td = res_ref.shape[0]
    texts = tk_ref.shape[0]
    share = -(-texts // groups)
    keys = heads * tok
    allk = kaug.shape[0]
    tpad = allk - keys
    per = tok // BS
    b = lax.axis_index("blk")
    j = lax.axis_index("head")
    z, r = b % heads, b // heads
    side, core = j // 2, j % 2

    barrier = pltpu.get_barrier_semaphore()
    close = (z * 2 // heads + r) % 2
    for i in range(1, heads):
        pl.semaphore_signal(barrier, inc=1, device_id=(r * heads + partner(z, i), j), device_id_type=MESH)

    @pl.when(close == 1)
    def _():
        for i in range(heads):
            to = (lax.rem(r + 1, groups) * heads + partner(z, i), j)
            pl.semaphore_signal(barrier, inc=1, device_id=to, device_id_type=MESH)

    count = heads - 1 + heads // 2 + nh - 1
    for k in range(1, nh):
        pl.semaphore_signal(barrier, inc=1, device_id=(b, lax.rem(j + k, nh)), device_id_type=MESH)

    local = []
    for s, (src, dst) in enumerate(
        ((v_ref, vin), (q_ref, qin), (k_ref, kin), (tk_ref, tkin), (tv_ref, tvin),
         (img_in, img_ref), (gate_in, gate_ref),
         (w_ref, wfull.at[pl.ds(pl.multiple_of(j * wrows, wrows), wrows)]), (res_ref, resv))
    ):
        copy = pltpu.make_async_copy(src, dst, l_sem.at[s])
        copy.start()
        local.append(copy)

    def remote(src, dst, ss, rs, to):
        return pltpu.make_async_remote_copy(
            src_ref=src, dst_ref=dst, send_sem=ss, recv_sem=rs, device_id=to, device_id_type=MESH
        )

    def go(copy):
        copy.start()

    local[0].wait()
    vt[...] = jnp.transpose(vin[...])
    local[2].wait()
    for h in range(heads):
        c = slice(h * HD, (h + 1) * HD)
        kh = kin[:, c]
        ks[h] = jnp.concatenate([kh[:half], kh[half:]], axis=1)
    local[1].wait()
    qt[...] = jnp.transpose(qin[...]) * BF16(HD ** -0.5)

    pl.semaphore_wait(barrier, count)

    def hrows(h):
        return pl.ds(pl.multiple_of(h * HD, HD), HD)

    def send_k(i):
        other = partner(z, i)
        go(remote(ks.at[other], kr.at[i], k_send, k_recv.at[i], (r * heads + other, j)))

    def send_v(i):
        other = partner(z, i)
        go(remote(vt.at[hrows(other)], va.at[pl.ds(0, HD), pl.ds(i * tok, tok)], v_send, v_recv,
                  (r * heads + other, j)))

    flip = close * (heads // 2)
    near = lax.rem(z + flip, heads)

    def send_q(k, i):
        at = partner(flip, i) if k else i
        other = partner(near, i) if k else partner(z, i)
        pos = (groups - k) % groups * heads + at
        go(remote(qt.at[hrows(other)], qa.at[pos, pl.ds(0, HD)], q_send, q_recv.at[pos],
                  (lax.rem(r + k, groups) * heads + other, j)))

    def send_cross(part):
        for k in range(1, groups):
            for i in part:
                send_q(k, i)

    def send_within(part):
        for i in part:
            send_q(0, i)

    def wrow(owner):
        return wfull.at[pl.ds(pl.multiple_of(owner * wrows, wrows), wrows)]

    sib = side * 2 + 1 - core
    go(remote(w_ref, wrow(j), ws_send, w_recv.at[j], (b, sib)))

    def arrived_w(owner):
        remote(w_ref, wrow(owner), ws_send, w_recv.at[owner], (b, sib)).wait_recv()

    def cross_w(src, owner):
        for k in range(1, nh // 2):
            to = lax.rem(side + k, nh // 2) * 2 + core
            go(remote(src, wrow(owner), wx_send, w_recv.at[owner], (b, to)))

    partners = list(range(heads // 2, heads)) + list(range(1, heads // 2))
    for i in partners:
        send_k(i)
    for i in partners:
        send_v(i)
    send_cross(range(heads // 2))
    send_within(range(1, heads // 2))

    @pl.when(close == 1)
    def _():
        send_within(range(heads // 2, heads))

    @pl.when(core == 1)
    def _():
        cross_w(w_ref, j)

    lane = lax.broadcasted_iota(jnp.int32, (16, LANES), 1)
    low_f = (lane < HD).astype(F32)
    low = low_f.astype(BF16)[:1]

    def onehot(image):
        return jnp.where(lane == HD + image, 1.0, 0.0).astype(BF16)[:1]

    local[5].wait()
    srow = lax.broadcasted_iota(jnp.int32, (QROWS - HD, BS), 0)
    for pos in range(n):
        first = (lax.rem(r + pos // heads, groups) * heads + partner(z, pos % heads)) * per
        for p in range(per):
            mask = jnp.where(srow == img_ref[first + p], 0.0, NEG).astype(BF16)
            qa[pos, pl.ds(HD, QROWS - HD), pl.ds(p * BS, BS)] = mask
    qa[0, pl.ds(0, HD), :] = qt[hrows(z), :]
    va[pl.ds(0, HD), pl.ds(0, tok)] = vt[hrows(z), :]
    va[pl.ds(HD, VROWS - HD), :] = jnp.ones((VROWS - HD, allk), BF16)

    local[3].wait()
    local[4].wait()
    traw[...] = jnp.zeros_like(traw)
    for h in range(heads):
        c = slice(h * HD, (h + 1) * HD)

        @pl.when(z == h)
        def _():
            traw[pl.ds(0, texts), :] = jnp.concatenate([tkin[:, c], tvin[:, c]], axis=1).astype(F32)

    span = -(-tpad // LANES) * LANES
    raw = traw[pl.ds(r * share, span), :]
    trow = lax.broadcasted_iota(jnp.int32, raw.shape, 0)
    tlane = lax.broadcasted_iota(jnp.int32, raw.shape, 1)
    timg = jnp.zeros_like(trow)
    for i in range(1, images + 1):
        timg += (trow + r * share >= i * TEXT).astype(jnp.int32)
    timg = jnp.where(trow < share, timg, images)
    taug = jnp.where(tlane < HD, raw, jnp.where(tlane == HD + timg, 1.0, 0.0)).astype(BF16)
    kaug[pl.ds(keys, tpad), :] = taug[:tpad]
    va[pl.ds(0, HD), pl.ds(keys, tpad)] = jnp.transpose(raw)[HD:, :tpad].astype(BF16)

    def load_k(i):
        first = (r * heads + partner(z, i)) * per
        for p in range(per):
            at = (p * BS) % half
            x = ks[z, pl.ds(at, BS), :] if i == 0 else kr[i, pl.ds(at, BS), :]
            if p * BS >= half:
                x = pltpu.roll(x.astype(F32), HD, 1).astype(BF16)
            kaug[pl.ds(i * tok + p * BS, BS), :] = x * low + onehot(img_ref[first + p])

    def blk(d, place):
        return lax.rem(r + d, groups) * heads + place

    own = [(i, blk(0, partner(z, i))) for i in range(heads)]
    cross = [
        (d * heads + partner(flip, i), blk(d, partner(near, i)))
        for d in range(1, groups) for i in range(heads)
    ]
    def arrive(pos):
        remote(qt.at[pl.ds(0, HD)], qa.at[pos, pl.ds(0, HD)], q_send, q_recv.at[pos], (b, sib)).wait_recv()

    load_k(0)
    for i in partners:
        remote(ks.at[0], kr.at[i], k_send, k_recv.at[i], (b, sib)).wait_recv()
        load_k(i)

    @pl.when(close == 1)
    def _():
        arrive(cross[0][0])
        to = (r * heads + partner(z, heads // 2), j)
        pl.semaphore_signal(told, inc=1, device_id=to, device_id_type=MESH)

    @pl.when(close == 0)
    def _():
        pl.semaphore_wait(told, 1)

    send_cross(range(heads // 2, heads))

    @pl.when(close == 0)
    def _():
        send_within(range(heads // 2, heads))

    order = own[:1] + [
        tuple(close * u + (1 - close) * v for u, v in zip(one, two))
        for one, two in zip(cross + own[1:], own[1:] + cross[len(cross) // 2:] + cross[:len(cross) // 2])
    ]

    def scores(pos, slot, low, width):
        c = pl.ds(low, width)
        s = jnp.dot(kaug[...], qa[pos, :, c], preferred_element_type=F32)
        sb[slot, :, c] = s
        mb[slot, :, c] = jnp.broadcast_to(jnp.max(s, axis=0, keepdims=True), (mb.shape[1], width))

    def attend(pos, slot, low, width):
        c = pl.ds(low, width)
        top = mb[slot, pl.ds(0, 1), c]
        p = jnp.exp(sb[slot, :, c] - top).astype(BF16)
        o = jnp.dot(va[...], p, preferred_element_type=F32)
        den = o[HD:HD + 1]
        y = (o[:HD] / den).astype(BF16)
        level = top + jnp.log(den)
        for d in range(width // td):
            osend[pos * nh + low // td + d] = y[:, d * td:(d + 1) * td]
            lsend[pos * nh + low // td + d] = level[:, d * td:(d + 1) * td]

    mine = (j * heads + z) * groups + r

    def give(pos, owner, dests):
        for dest in dests:
            at = pos * nh + dest
            go(remote(osend.at[at], orecv.at[mine], o_send, o_recv, (owner, dest)))
            go(remote(lsend.at[at], lrecv.at[mine], e_send, e_recv, (owner, dest)))

    def relay_w():
        @pl.when(core == 1)
        def _():
            for k in range(1, nh // 2):
                for c in range(2):
                    owner = lax.rem(side + k, nh // 2) * 2 + 1 - c
                    arrived_w(owner)
                    go(remote(wrow(owner), wrow(owner), ws_send, w_recv.at[owner], (b, sib)))

    scores(0, 0, 0, tok)
    rest = va.at[pl.ds(0, HD), pl.ds(tok, keys - tok)]
    remote(rest, rest, v_send, v_recv, (b, sib)).wait_recv()
    @pl.when(core == 1)
    def _():
        arrived_w(sib)
        cross_w(wrow(sib), sib)


    for t, (pos, owner) in enumerate(order):
        if t + 1 < n:
            if t:
                arrive(order[t + 1][0])
            else:
                pl.when(close == 0)(lambda: arrive(own[1][0]))
            scores(order[t + 1][0], (t + 1) % 2, 0, tok)
        attend(pos, t % 2, 0, tok)
        if t == 0:
            orecv[mine] = osend[j]
            lrecv[mine] = lsend[j]
        turns = [(k + nh // 2) % nh for k in range(nh)]
        give(pos, owner, [lax.rem(j + k, nh) for k in turns if k or t])
    relay_w()

    local[6].wait()
    local[7].wait()
    local[8].wait()
    most = pl.ds(0, n * nh - 1)
    outs = remote(osend.at[most], orecv.at[most], o_send, o_recv, (b, sib))
    ends = remote(lsend.at[most], lrecv.at[most], e_send, e_recv, (b, sib))
    outs.wait_recv()
    ends.wait_recv()
    for h in range(heads * nh):
        levels = [lrecv[h * groups + g] for g in range(groups)]
        top = functools.reduce(jnp.maximum, levels)
        ws = [jnp.exp(x - top) for x in levels]
        total = functools.reduce(jnp.add, ws)
        parts = [orecv[h * groups + g].astype(F32) * (ws[g] / total) for g in range(groups)]
        mixed[pl.ds(h * HD, HD), :] = functools.reduce(jnp.add, parts).astype(BF16)
    @pl.when(core == 0)
    def _():
        arrived_w(sib)
        for k in range(1, nh // 2):
            for c in range(2):
                arrived_w(lax.rem(side + k, nh // 2) * 2 + c)

    attended = jnp.transpose(mixed[...])
    unit = min(td, BS)
    width = 256
    for t in range(out_ref.shape[1] // width):
        c = pl.ds(t * width, width)
        y = jnp.dot(attended, wfull[:, c], preferred_element_type=F32)
        for u in range(td // unit):
            image = img_ref[(b * tok + j * td + u * unit) // BS]
            gate = jnp.zeros((1, width), F32)
            for m in range(images):
                gate = jnp.where(image == m, gate_ref[pl.ds(m, 1), c], gate)
            rows = pl.ds(u * unit, unit)
            part = y[u * unit:(u + 1) * unit]
            out_ref[rows, c] = (resv[rows, c].astype(F32) + gate * part).astype(BF16)

    outs.wait_send()
    ends.wait_send()
    most = pl.ds(0, heads - 1)
    remote(ks.at[most], kr.at[most], k_send, k_recv.at[0], (b, sib)).wait_send()
    remote(rest, rest, v_send, v_recv, (b, sib)).wait_send()
    most = pl.ds(0, n - 1)
    part = qa.at[most, pl.ds(0, HD)]
    remote(part, part, q_send, q_recv.at[0], (b, sib)).wait_send()
    remote(w_ref, wrow(j), ws_send, w_recv.at[j], (b, sib)).wait_send()

    @pl.when(core == 1)
    def _():
        part = wfull.at[pl.ds(0, (nh - 2) * wrows)]
        remote(part, part, wx_send, w_recv.at[0], (b, sib)).wait_send()
        remote(part, part, ws_send, w_recv.at[0], (b, sib)).wait_send()


def split_call(n, nh, *args):
    q, k, v, tk, tv, block_image, gate, res, w = args
    tok, cols = q.shape
    heads = cols // HD
    groups = n // heads
    td = res.shape[0]
    share = -(-tk.shape[0] // groups)
    tpad = -(-share // 16) * 16
    span = -(-tpad // LANES) * LANES
    keys = heads * tok + tpad
    vm = pl.BlockSpec(memory_space=pltpu.VMEM)
    hbm = pl.BlockSpec(memory_space=pltpu.HBM)
    dma = pltpu.SemaphoreType.DMA
    return pl.pallas_call(
        functools.partial(split_kernel, n, nh),
        out_shape=pltpu.VMEM(res.shape, BF16),
        in_specs=[hbm] * 9,
        out_specs=vm,
        scratch_shapes=[
            pltpu.VMEM(q.shape, BF16), pltpu.VMEM(k.shape, BF16), pltpu.VMEM(v.shape, BF16),
            pltpu.VMEM(tk.shape, BF16), pltpu.VMEM(tv.shape, BF16),
            pltpu.SMEM(block_image.shape, jnp.int32), pltpu.VMEM(gate.shape, F32),
            pltpu.VMEM((cols, tok), BF16), pltpu.VMEM((cols, tok), BF16),
            pltpu.VMEM((heads, tok // 2, LANES), BF16), pltpu.VMEM((heads, tok // 2, LANES), BF16),
            pltpu.VMEM((n, QROWS, tok), BF16),
            pltpu.VMEM((keys, LANES), BF16),
            pltpu.VMEM((VROWS, keys), BF16),
            pltpu.VMEM(((groups - 1) * share + max(span, tk.shape[0]) + 8, LANES), F32),
            pltpu.VMEM((2, keys, tok), F32),
            pltpu.VMEM((2, 8, tok), F32),
            pltpu.VMEM((n * nh, HD, td), BF16),
            pltpu.VMEM((n * nh, 1, td), F32),
            pltpu.VMEM((n * nh, HD, td), BF16),
            pltpu.VMEM((n * nh, 1, td), F32),
            pltpu.VMEM((heads * nh * HD, td), BF16),
            pltpu.VMEM((w.shape[0] * nh, w.shape[1]), BF16),
            pltpu.VMEM(res.shape, BF16),
            dma, dma((n,)), dma, dma((heads,)), dma, dma,
            dma, dma, dma((nh,)), dma, dma, dma, dma, dma((9,)), pltpu.SemaphoreType.REGULAR,
        ],
        compiler_params=pltpu.CompilerParams(
            collective_id=0, has_side_effects=True, vmem_limit_bytes=40 * 1024 * 1024
        ),
    )(*(pltpu.with_memory_space_constraint(x, pltpu.HBM) for x in args))


def solution(mesh):
    n, nh = mesh.shape["blk"], mesh.shape["head"]

    def on_device(q, k, v, tk, tv, block_image, gate, res, w):
        tok, cols = q.shape
        heads = cols // HD
        groups = n // heads
        td = res.shape[0]
        rows = heads * tok
        if groups == 2 and heads > 1 and td % LANES == 0 and tok % (2 * BS) == 0:
            return split_call(n, nh, q, k, v, tk, tv, block_image, gate, res, w)
        upad = -(-tk.shape[0] // LANES) * LANES
        vm = pl.BlockSpec(memory_space=pltpu.VMEM)
        anyw = pl.BlockSpec(memory_space=pl.ANY)
        dma = pltpu.SemaphoreType.DMA
        return pl.pallas_call(
            functools.partial(kernel, n, nh),
            out_shape=jax.ShapeDtypeStruct(res.shape, BF16),
            in_specs=[vm, vm, vm, vm, vm, pl.BlockSpec(memory_space=pltpu.SMEM), vm, anyw, anyw],
            out_specs=vm,
            scratch_shapes=[
                pltpu.VMEM((heads, tok // 2, LANES), BF16),
                pltpu.VMEM((heads, tok, LANES), BF16),
                pltpu.VMEM((heads, tok // 2, LANES), BF16),
                pltpu.VMEM((n, tok, LANES), BF16),
                pltpu.VMEM((upad, LANES), F32),
                pltpu.VMEM((rows, LANES), BF16),
                pltpu.VMEM((n * tok, LANES), BF16),
                pltpu.VMEM((n * tok, LANES), BF16),
                pltpu.VMEM((upad, LANES), BF16),
                pltpu.VMEM((upad, LANES), BF16),
                pltpu.VMEM((rows, LANES), F32),
                pltpu.VMEM((rows, LANES), F32),
                pltpu.VMEM((heads * nh, td // 2, LANES), BF16),
                pltpu.VMEM((heads * nh, td // 2, LANES), BF16),
                pltpu.VMEM((td, heads * nh * HD), BF16),
                pltpu.VMEM((w.shape[0] * nh, w.shape[1]), BF16),
                pltpu.VMEM(res.shape, BF16),
                dma((heads,)), dma((heads,)), dma((n,)), dma((n,)),
                dma((nh,)), dma((nh,)), dma((nh,)), dma((heads * nh,)), dma((heads * nh,)), dma((2,)),
            ],
            compiler_params=pltpu.CompilerParams(
                collective_id=0, has_side_effects=True, vmem_limit_bytes=60 * 1024 * 1024
            ),
        )(q, k, v, tk, tv, block_image, gate, res, w)

    placed = (
        P("blk", "head"), P("blk", "head"), P("blk", "head"), P(None, "head"), P(None, "head"),
        P(), P(), P(("blk", "head"), None), P("head", None),
    )
    return jax.shard_map(
        on_device, mesh=mesh, in_specs=placed, out_specs=P(("blk", "head"), None), check_vma=False
    )
```

```python
import functools

import jax
import jax.numpy as jnp
from jax import lax
from jax.experimental import pallas as pl
from jax.experimental.pallas import tpu as pltpu
from jax.sharding import PartitionSpec as P

HD = 64
TEXT = 154
BS = 128
NEG = -1e30
LANES = 128
QTILE = 512
KEYS = 1024
MESH = pl.DeviceIdType.MESH
F32 = jnp.float32
BF16 = jnp.bfloat16


def partner(z, i):
    out, bit = z, 1
    while bit <= i:
        if i & bit:
            out = out + bit - 2 * bit * ((out // bit) % 2)
        bit *= 2
    return out


def kernel(
    n, nh, q_ref, k_ref, v_ref, tk_ref, tv_ref, img_ref, gate_ref, res_ref, w_ref, out_ref,
    qs, kvs, qr, kvr, traw, qaug, kaug, kval, taug, tval, best, accum, osend, orecv, mixed, wfull, resv,
    q_send, q_recv, kv_send, kv_recv, wx_send, ws_send, w_recv, o_send, o_recv, l_sem,
):
    tok, cols = q_ref.shape
    heads = cols // HD
    groups = n // heads
    half = tok // 2
    images = gate_ref.shape[0]
    wrows = w_ref.shape[0]
    td = res_ref.shape[0]
    texts = tk_ref.shape[0]
    per = tok // BS
    b = lax.axis_index("blk")
    j = lax.axis_index("head")
    z, r = b % heads, b // heads
    side, core = j // 2, j % 2

    barrier = pltpu.get_barrier_semaphore()
    count = 0
    for i in range(heads):
        for k in range(nh):
            if i or k:
                to = (r * heads + partner(z, i), lax.rem(j + k, nh))
                pl.semaphore_signal(barrier, inc=1, device_id=to, device_id_type=MESH)
                count += 1
    for k in range(1, groups):
        for i in range(heads):
            to = (lax.rem(r + k, groups) * heads + partner(z, i), j)
            pl.semaphore_signal(barrier, inc=1, device_id=to, device_id_type=MESH)
            count += 1

    w_here = pltpu.make_async_copy(w_ref, wfull.at[pl.ds(pl.multiple_of(j * wrows, wrows), wrows)], l_sem.at[0])
    w_here.start()
    res_here = pltpu.make_async_copy(res_ref, resv, l_sem.at[1])
    res_here.start()

    for h in range(heads):
        c = slice(h * HD, (h + 1) * HD)
        q = q_ref[:, c] * BF16(HD ** -0.5)
        qs[h] = jnp.concatenate([q[:half], q[half:]], axis=1)
        kvs[h] = jnp.concatenate([k_ref[:, c], v_ref[:, c]], axis=1)

    pl.semaphore_wait(barrier, count)

    def remote(src, dst, ss, rs, to):
        return pltpu.make_async_remote_copy(
            src_ref=src, dst_ref=dst, send_sem=ss, recv_sem=rs, device_id=to, device_id_type=MESH
        )

    sent = []

    def go(copy):
        copy.start()
        sent.append(copy)

    def wrow(owner):
        return wfull.at[pl.ds(pl.multiple_of(owner * wrows, wrows), wrows)]

    def send_kv(i, k):
        other = partner(z, i)
        pos = (groups - k) % groups * heads + i
        go(remote(kvs.at[other], kvr.at[pos], kv_send.at[pos], kv_recv.at[pos],
                  (lax.rem(r + k, groups) * heads + other, j)))

    for i in range(1, heads):
        other = partner(z, i)
        go(remote(qs.at[other], qr.at[i], q_send.at[i], q_recv.at[i], (r * heads + other, j)))
    for i in range(1, heads):
        send_kv(i, 0)
    for i in range(heads):
        for k in range(1, groups):
            send_kv(i, k)
    sib = side * 2 + 1 - core
    go(remote(w_ref, wrow(j), ws_send.at[0], w_recv.at[j], (b, sib)))
    for k in range(1, nh // 2):
        to = lax.rem(side + k, nh // 2) * 2 + core
        go(remote(w_ref, wrow(j), wx_send.at[k], w_recv.at[j], (b, to)))

    lane = lax.broadcasted_iota(jnp.int32, (16, LANES), 1)
    low_f = (lane < HD).astype(F32)
    low = low_f.astype(BF16)[:1]
    high = (1.0 - low_f).astype(BF16)[:1]

    def onehot(image):
        return jnp.where(lane == HD + image, 1.0, 0.0).astype(BF16)[:1]

    def others(image):
        return jnp.where((lane < HD) | (lane == HD + image), 0.0, NEG).astype(BF16)[:1]

    traw[...] = jnp.zeros_like(traw)
    for h in range(heads):
        c = slice(h * HD, (h + 1) * HD)

        @pl.when(z == h)
        def _():
            traw[pl.ds(0, texts), :] = jnp.concatenate([tk_ref[:, c], tv_ref[:, c]], axis=1).astype(F32)

    trow = lax.broadcasted_iota(jnp.int32, traw.shape, 0)
    tlane = lax.broadcasted_iota(jnp.int32, traw.shape, 1)
    timg = jnp.zeros_like(trow)
    for i in range(1, images + 1):
        timg += (trow >= i * TEXT).astype(jnp.int32)
    raw = traw[...]
    taug[...] = jnp.where(tlane < HD, raw, jnp.where(tlane == HD + timg, 1.0, 0.0)).astype(BF16)
    tval[...] = jnp.where(tlane < HD, 1.0, raw).astype(BF16)

    def load_q(i):
        src = qs.at[z] if i == 0 else qr.at[i]
        first = (r * heads + partner(z, i)) * per
        for p in range(per):
            at = (p * BS) % half
            x = src[pl.ds(at, BS), :]
            if p * BS >= half:
                x = pltpu.roll(x.astype(F32), HD, 1).astype(BF16)
            qaug[pl.ds(i * tok + p * BS, BS), :] = x * low + others(img_ref[first + p])

    def load_kv(pos):
        first = (lax.rem(r + pos // heads, groups) * heads + partner(z, pos % heads)) * per
        for p in range(per):
            x = kvr[pos, pl.ds(p * BS, BS), :]
            rows = pl.ds(pos * tok + p * BS, BS)
            kaug[rows, :] = x * low + onehot(img_ref[first + p])
            kval[rows, :] = x * high + low

    def absorb(keys, vals, start, count, fresh):
        def body(t, carry):
            rows = pl.ds(pl.multiple_of(start + t * QTILE, QTILE), QTILE)
            s = lax.dot_general(qaug[rows, :], keys(), (((1,), (1,)), ((), ())), preferred_element_type=F32)
            top = jnp.broadcast_to(jnp.max(s, axis=1, keepdims=True), (QTILE, LANES))
            if not fresh:
                old = best[rows, :]
                top = jnp.maximum(old, top)
            wide = jnp.concatenate([top] * (s.shape[1] // LANES), axis=1)
            p = jnp.exp(s - wide).astype(BF16)
            add = jnp.dot(p, vals(), preferred_element_type=F32)
            if fresh:
                accum[rows, :] = add
            else:
                accum[rows, :] = accum[rows, :] * jnp.exp(old - top) + add
            best[rows, :] = top
            return carry

        lax.fori_loop(0, count // QTILE, body, 0, unroll=1)

    kvr[0] = kvs[z]
    for i in range(heads):
        if i:
            remote(qs.at[0], qr.at[i], q_send.at[i], q_recv.at[i], (b, sib)).wait_recv()
        load_q(i)
        absorb(lambda: taug[...], lambda: tval[...], i * tok, tok, True)

    join = max(1, min(heads, KEYS // tok))

    def arrive(pos):
        remote(kvs.at[0], kvr.at[pos], kv_send.at[0], kv_recv.at[pos], (b, sib)).wait_recv()

    def relay_w():
        for k in range(1, nh // 2):
            owner = lax.rem(side + nh // 2 - k, nh // 2) * 2 + core
            remote(w_ref, wrow(owner), ws_send.at[k], w_recv.at[owner], (b, sib)).wait_recv()
            go(remote(wrow(owner), wrow(owner), ws_send.at[k], w_recv.at[owner], (b, sib)))

    def finish(i):
        low2 = lax.broadcasted_iota(jnp.int32, (td // 2, LANES), 1) < HD
        to_blk = r * heads + partner(z, i)
        slot = j * heads + z
        for k in range(nh):
            dest = lax.rem(j + k, nh)
            base = pl.multiple_of(i * tok + dest * td, td)
            one = accum[pl.ds(base, td // 2), :]
            two = accum[pl.ds(base + td // 2, td // 2), :]
            one_r, two_r = pltpu.roll(one, HD, 1), pltpu.roll(two, HD, 1)
            y = (jnp.where(low2, one_r, two) / jnp.where(low2, one, two_r)).astype(BF16)
            if i == 0 and k == 0:
                orecv[slot] = y
            else:
                osend[i * nh + k] = y
                go(remote(osend.at[i * nh + k], orecv.at[slot], o_send.at[i * nh + k], o_recv.at[slot],
                          (to_blk, dest)))

    for g in range(0, n, join):
        for pos in range(g, g + join):
            if pos:
                arrive(pos)
            load_kv(pos)
        at = pl.ds(g * tok, join * tok)
        args = (lambda: kaug[at, :], lambda: kval[at, :])
        if g + join == n:
            relay_w()
            for s in reversed(range(heads)):
                absorb(*args, s * tok, tok, False)
                finish(s)
        else:
            absorb(*args, 0, heads * tok, False)

    w_here.wait()
    res_here.wait()
    for k in range(nh // 2):
        owner = lax.rem(side + nh // 2 - k, nh // 2) * 2 + 1 - core
        remote(w_ref, wrow(owner), ws_send.at[k], w_recv.at[owner], (b, sib)).wait_recv()
    for i in range(heads):
        for k in range(nh):
            if i or k:
                slot = lax.rem(j + k, nh) * heads + partner(z, i)
                remote(osend.at[0], orecv.at[slot], o_send.at[0], o_recv.at[slot], (b, sib)).wait_recv()
    low2 = lax.broadcasted_iota(jnp.int32, (td // 2, LANES), 1) < HD
    for p in range(heads * nh // 2):
        even, odd = orecv[2 * p].astype(F32), orecv[2 * p + 1].astype(F32)
        c = pl.ds(p * LANES, LANES)
        mixed[pl.ds(0, td // 2), c] = jnp.where(low2, even, pltpu.roll(odd, HD, 1)).astype(BF16)
        mixed[pl.ds(td // 2, td // 2), c] = jnp.where(low2, pltpu.roll(even, HD, 1), odd).astype(BF16)

    unit = min(td, BS)
    width = 256
    for t in range(out_ref.shape[1] // width):
        c = pl.ds(t * width, width)
        y = jnp.dot(mixed[...], wfull[:, c], preferred_element_type=F32)
        for u in range(td // unit):
            image = img_ref[(b * tok + j * td + u * unit) // BS]
            gate = jnp.zeros((1, width), F32)
            for m in range(images):
                gate = jnp.where(image == m, gate_ref[pl.ds(m, 1), c], gate)
            rows = pl.ds(u * unit, unit)
            part = y[u * unit:(u + 1) * unit]
            out_ref[rows, c] = (resv[rows, c].astype(F32) + gate * part).astype(BF16)

    for copy in sent:
        copy.wait_send()


QROWS = 128
VROWS = 80


def split_kernel(
    n, nh, q_ref, k_ref, v_ref, tk_ref, tv_ref, img_in, gate_in, res_ref, w_ref, out_ref,
    qin, kin, vin, tkin, tvin, img_ref, gate_ref, qt, vt, ks, kr, qa, kaug, va, traw, sb, mb, osend, lsend, orecv, lrecv,
    mixed, wfull, resv,
    q_send, q_recv, k_send, k_recv, v_send, v_recv, wx_send, ws_send, w_recv, o_send, o_recv, e_send, e_recv, l_sem, told,
):
    tok, cols = q_ref.shape
    heads = cols // HD
    groups = n // heads
    half = tok // 2
    images = gate_ref.shape[0]
    wrows = w_ref.shape[0]
    td = res_ref.shape[0]
    texts = tk_ref.shape[0]
    share = -(-texts // groups)
    keys = heads * tok
    allk = kaug.shape[0]
    tpad = allk - keys
    per = tok // BS
    b = lax.axis_index("blk")
    j = lax.axis_index("head")
    z, r = b % heads, b // heads
    side, core = j // 2, j % 2

    barrier = pltpu.get_barrier_semaphore()
    close = (z * 2 // heads + r) % 2
    for i in range(1, heads):
        pl.semaphore_signal(barrier, inc=1, device_id=(r * heads + partner(z, i), j), device_id_type=MESH)

    @pl.when(close == 1)
    def _():
        for i in range(heads):
            to = (lax.rem(r + 1, groups) * heads + partner(z, i), j)
            pl.semaphore_signal(barrier, inc=1, device_id=to, device_id_type=MESH)

    count = heads - 1 + heads // 2 + nh - 1
    for k in range(1, nh):
        pl.semaphore_signal(barrier, inc=1, device_id=(b, lax.rem(j + k, nh)), device_id_type=MESH)

    local = []
    for s, (src, dst) in enumerate(
        ((v_ref, vin), (q_ref, qin), (k_ref, kin), (tk_ref, tkin), (tv_ref, tvin),
         (img_in, img_ref), (gate_in, gate_ref),
         (w_ref, wfull.at[pl.ds(pl.multiple_of(j * wrows, wrows), wrows)]), (res_ref, resv))
    ):
        copy = pltpu.make_async_copy(src, dst, l_sem.at[s])
        copy.start()
        local.append(copy)

    def remote(src, dst, ss, rs, to):
        return pltpu.make_async_remote_copy(
            src_ref=src, dst_ref=dst, send_sem=ss, recv_sem=rs, device_id=to, device_id_type=MESH
        )

    def go(copy):
        copy.start()

    local[0].wait()
    vt[...] = jnp.transpose(vin[...])
    local[2].wait()
    for h in range(heads):
        c = slice(h * HD, (h + 1) * HD)
        kh = kin[:, c]
        ks[h] = jnp.concatenate([kh[:half], kh[half:]], axis=1)
    local[1].wait()
    qt[...] = jnp.transpose(qin[...]) * BF16(HD ** -0.5)

    pl.semaphore_wait(barrier, count)

    def hrows(h):
        return pl.ds(pl.multiple_of(h * HD, HD), HD)

    def send_k(i):
        other = partner(z, i)
        go(remote(ks.at[other], kr.at[i], k_send, k_recv.at[i], (r * heads + other, j)))

    def send_v(i):
        other = partner(z, i)
        go(remote(vt.at[hrows(other)], va.at[pl.ds(0, HD), pl.ds(i * tok, tok)], v_send, v_recv,
                  (r * heads + other, j)))

    flip = close * (heads // 2)
    near = lax.rem(z + flip, heads)

    def send_q(k, i):
        at = partner(flip, i) if k else i
        other = partner(near, i) if k else partner(z, i)
        pos = (groups - k) % groups * heads + at
        go(remote(qt.at[hrows(other)], qa.at[pos, pl.ds(0, HD)], q_send, q_recv.at[pos],
                  (lax.rem(r + k, groups) * heads + other, j)))

    def send_cross(part):
        for k in range(1, groups):
            for i in part:
                send_q(k, i)

    def send_within(part):
        for i in part:
            send_q(0, i)

    def wrow(owner):
        return wfull.at[pl.ds(pl.multiple_of(owner * wrows, wrows), wrows)]

    sib = side * 2 + 1 - core
    go(remote(w_ref, wrow(j), ws_send, w_recv.at[j], (b, sib)))

    def arrived_w(owner):
        remote(w_ref, wrow(owner), ws_send, w_recv.at[owner], (b, sib)).wait_recv()

    def cross_w(src, owner):
        for k in range(1, nh // 2):
            to = lax.rem(side + k, nh // 2) * 2 + core
            go(remote(src, wrow(owner), wx_send, w_recv.at[owner], (b, to)))

    partners = list(range(heads // 2, heads)) + list(range(1, heads // 2))
    for i in partners:
        send_k(i)
    for i in partners:
        send_v(i)
    send_cross(range(heads // 2))
    send_within(range(1, heads // 2))

    @pl.when(close == 1)
    def _():
        send_within(range(heads // 2, heads))

    @pl.when(core == 1)
    def _():
        cross_w(w_ref, j)

    lane = lax.broadcasted_iota(jnp.int32, (16, LANES), 1)
    low_f = (lane < HD).astype(F32)
    low = low_f.astype(BF16)[:1]

    def onehot(image):
        return jnp.where(lane == HD + image, 1.0, 0.0).astype(BF16)[:1]

    local[5].wait()
    srow = lax.broadcasted_iota(jnp.int32, (QROWS - HD, BS), 0)
    for pos in range(n):
        first = (lax.rem(r + pos // heads, groups) * heads + partner(z, pos % heads)) * per
        for p in range(per):
            mask = jnp.where(srow == img_ref[first + p], 0.0, NEG).astype(BF16)
            qa[pos, pl.ds(HD, QROWS - HD), pl.ds(p * BS, BS)] = mask
    qa[0, pl.ds(0, HD), :] = qt[hrows(z), :]
    va[pl.ds(0, HD), pl.ds(0, tok)] = vt[hrows(z), :]
    va[pl.ds(HD, VROWS - HD), :] = jnp.ones((VROWS - HD, allk), BF16)

    local[3].wait()
    local[4].wait()
    traw[...] = jnp.zeros_like(traw)
    for h in range(heads):
        c = slice(h * HD, (h + 1) * HD)

        @pl.when(z == h)
        def _():
            traw[pl.ds(0, texts), :] = jnp.concatenate([tkin[:, c], tvin[:, c]], axis=1).astype(F32)

    span = -(-tpad // LANES) * LANES
    raw = traw[pl.ds(r * share, span), :]
    trow = lax.broadcasted_iota(jnp.int32, raw.shape, 0)
    tlane = lax.broadcasted_iota(jnp.int32, raw.shape, 1)
    timg = jnp.zeros_like(trow)
    for i in range(1, images + 1):
        timg += (trow + r * share >= i * TEXT).astype(jnp.int32)
    timg = jnp.where(trow < share, timg, images)
    taug = jnp.where(tlane < HD, raw, jnp.where(tlane == HD + timg, 1.0, 0.0)).astype(BF16)
    kaug[pl.ds(keys, tpad), :] = taug[:tpad]
    va[pl.ds(0, HD), pl.ds(keys, tpad)] = jnp.transpose(raw)[HD:, :tpad].astype(BF16)

    def load_k(i):
        first = (r * heads + partner(z, i)) * per
        for p in range(per):
            at = (p * BS) % half
            x = ks[z, pl.ds(at, BS), :] if i == 0 else kr[i, pl.ds(at, BS), :]
            if p * BS >= half:
                x = pltpu.roll(x.astype(F32), HD, 1).astype(BF16)
            kaug[pl.ds(i * tok + p * BS, BS), :] = x * low + onehot(img_ref[first + p])

    def blk(d, place):
        return lax.rem(r + d, groups) * heads + place

    own = [(i, blk(0, partner(z, i))) for i in range(heads)]
    cross = [
        (d * heads + partner(flip, i), blk(d, partner(near, i)))
        for d in range(1, groups) for i in range(heads)
    ]
    def arrive(pos):
        remote(qt.at[pl.ds(0, HD)], qa.at[pos, pl.ds(0, HD)], q_send, q_recv.at[pos], (b, sib)).wait_recv()

    load_k(0)
    for i in partners:
        remote(ks.at[0], kr.at[i], k_send, k_recv.at[i], (b, sib)).wait_recv()
        load_k(i)

    @pl.when(close == 1)
    def _():
        arrive(cross[0][0])
        to = (r * heads + partner(z, heads // 2), j)
        pl.semaphore_signal(told, inc=1, device_id=to, device_id_type=MESH)

    @pl.when(close == 0)
    def _():
        pl.semaphore_wait(told, 1)

    send_cross(range(heads // 2, heads))

    @pl.when(close == 0)
    def _():
        send_within(range(heads // 2, heads))

    order = own[:1] + [
        tuple(close * u + (1 - close) * v for u, v in zip(one, two))
        for one, two in zip(cross + own[1:], own[1:] + cross[len(cross) // 2:] + cross[:len(cross) // 2])
    ]

    def scores(pos, slot, low, width):
        c = pl.ds(low, width)
        s = jnp.dot(kaug[...], qa[pos, :, c], preferred_element_type=F32)
        sb[slot, :, c] = s
        mb[slot, :, c] = jnp.broadcast_to(jnp.max(s, axis=0, keepdims=True), (mb.shape[1], width))

    def attend(pos, slot, low, width):
        c = pl.ds(low, width)
        top = mb[slot, pl.ds(0, 1), c]
        p = jnp.exp(sb[slot, :, c] - top).astype(BF16)
        o = jnp.dot(va[...], p, preferred_element_type=F32)
        den = o[HD:HD + 1]
        y = (o[:HD] / den).astype(BF16)
        level = top + jnp.log(den)
        for d in range(width // td):
            osend[pos * nh + low // td + d] = y[:, d * td:(d + 1) * td]
            lsend[pos * nh + low // td + d] = level[:, d * td:(d + 1) * td]

    mine = (j * heads + z) * groups + r

    def give(pos, owner, dests):
        for dest in dests:
            at = pos * nh + dest
            go(remote(lsend.at[at], lrecv.at[mine], e_send, e_recv, (owner, dest)))
            go(remote(osend.at[at], orecv.at[mine], o_send, o_recv, (owner, dest)))

    def relay_w():
        @pl.when(core == 1)
        def _():
            for k in range(1, nh // 2):
                for c in range(2):
                    owner = lax.rem(side + k, nh // 2) * 2 + 1 - c
                    arrived_w(owner)
                    go(remote(wrow(owner), wrow(owner), ws_send, w_recv.at[owner], (b, sib)))

    scores(0, 0, 0, tok)
    rest = va.at[pl.ds(0, HD), pl.ds(tok, keys - tok)]
    remote(rest, rest, v_send, v_recv, (b, sib)).wait_recv()
    @pl.when(core == 1)
    def _():
        arrived_w(sib)
        cross_w(wrow(sib), sib)


    for t, (pos, owner) in enumerate(order):
        if t + 1 < n:
            if t:
                arrive(order[t + 1][0])
            else:
                pl.when(close == 0)(lambda: arrive(own[1][0]))
            scores(order[t + 1][0], (t + 1) % 2, 0, tok)
        attend(pos, t % 2, 0, tok)
        if t == 0:
            orecv[mine] = osend[j]
            lrecv[mine] = lsend[j]
        turns = [(k + nh // 2) % nh for k in range(nh)]
        give(pos, owner, [lax.rem(j + k, nh) for k in turns if k or t])
    relay_w()

    local[6].wait()
    local[7].wait()
    local[8].wait()
    most = pl.ds(0, n * nh - 1)
    outs = remote(osend.at[most], orecv.at[most], o_send, o_recv, (b, sib))
    ends = remote(lsend.at[most], lrecv.at[most], e_send, e_recv, (b, sib))
    outs.wait_recv()
    ends.wait_recv()
    for h in range(heads * nh):
        levels = [lrecv[h * groups + g] for g in range(groups)]
        top = functools.reduce(jnp.maximum, levels)
        ws = [jnp.exp(x - top) for x in levels]
        total = functools.reduce(jnp.add, ws)
        parts = [orecv[h * groups + g].astype(F32) * (ws[g] / total) for g in range(groups)]
        mixed[pl.ds(h * HD, HD), :] = functools.reduce(jnp.add, parts).astype(BF16)
    @pl.when(core == 0)
    def _():
        arrived_w(sib)
        for k in range(1, nh // 2):
            for c in range(2):
                arrived_w(lax.rem(side + k, nh // 2) * 2 + c)

    attended = jnp.transpose(mixed[...])
    unit = min(td, BS)
    width = 256
    for t in range(out_ref.shape[1] // width):
        c = pl.ds(t * width, width)
        y = jnp.dot(attended, wfull[:, c], preferred_element_type=F32)
        for u in range(td // unit):
            image = img_ref[(b * tok + j * td + u * unit) // BS]
            gate = jnp.zeros((1, width), F32)
            for m in range(images):
                gate = jnp.where(image == m, gate_ref[pl.ds(m, 1), c], gate)
            rows = pl.ds(u * unit, unit)
            part = y[u * unit:(u + 1) * unit]
            out_ref[rows, c] = (resv[rows, c].astype(F32) + gate * part).astype(BF16)

    outs.wait_send()
    ends.wait_send()
    most = pl.ds(0, heads - 1)
    remote(ks.at[most], kr.at[most], k_send, k_recv.at[0], (b, sib)).wait_send()
    remote(rest, rest, v_send, v_recv, (b, sib)).wait_send()
    most = pl.ds(0, n - 1)
    part = qa.at[most, pl.ds(0, HD)]
    remote(part, part, q_send, q_recv.at[0], (b, sib)).wait_send()
    remote(w_ref, wrow(j), ws_send, w_recv.at[j], (b, sib)).wait_send()

    @pl.when(core == 1)
    def _():
        part = wfull.at[pl.ds(0, (nh - 2) * wrows)]
        remote(part, part, wx_send, w_recv.at[0], (b, sib)).wait_send()
        remote(part, part, ws_send, w_recv.at[0], (b, sib)).wait_send()


def split_call(n, nh, *args):
    q, k, v, tk, tv, block_image, gate, res, w = args
    tok, cols = q.shape
    heads = cols // HD
    groups = n // heads
    td = res.shape[0]
    share = -(-tk.shape[0] // groups)
    tpad = -(-share // 16) * 16
    span = -(-tpad // LANES) * LANES
    keys = heads * tok + tpad
    vm = pl.BlockSpec(memory_space=pltpu.VMEM)
    hbm = pl.BlockSpec(memory_space=pltpu.HBM)
    dma = pltpu.SemaphoreType.DMA
    return pl.pallas_call(
        functools.partial(split_kernel, n, nh),
        out_shape=pltpu.VMEM(res.shape, BF16),
        in_specs=[hbm] * 9,
        out_specs=vm,
        scratch_shapes=[
            pltpu.VMEM(q.shape, BF16), pltpu.VMEM(k.shape, BF16), pltpu.VMEM(v.shape, BF16),
            pltpu.VMEM(tk.shape, BF16), pltpu.VMEM(tv.shape, BF16),
            pltpu.SMEM(block_image.shape, jnp.int32), pltpu.VMEM(gate.shape, F32),
            pltpu.VMEM((cols, tok), BF16), pltpu.VMEM((cols, tok), BF16),
            pltpu.VMEM((heads, tok // 2, LANES), BF16), pltpu.VMEM((heads, tok // 2, LANES), BF16),
            pltpu.VMEM((n, QROWS, tok), BF16),
            pltpu.VMEM((keys, LANES), BF16),
            pltpu.VMEM((VROWS, keys), BF16),
            pltpu.VMEM(((groups - 1) * share + max(span, tk.shape[0]) + 8, LANES), F32),
            pltpu.VMEM((2, keys, tok), F32),
            pltpu.VMEM((2, 8, tok), F32),
            pltpu.VMEM((n * nh, HD, td), BF16),
            pltpu.VMEM((n * nh, 1, td), F32),
            pltpu.VMEM((n * nh, HD, td), BF16),
            pltpu.VMEM((n * nh, 1, td), F32),
            pltpu.VMEM((heads * nh * HD, td), BF16),
            pltpu.VMEM((w.shape[0] * nh, w.shape[1]), BF16),
            pltpu.VMEM(res.shape, BF16),
            dma, dma((n,)), dma, dma((heads,)), dma, dma,
            dma, dma, dma((nh,)), dma, dma, dma, dma, dma((9,)), pltpu.SemaphoreType.REGULAR,
        ],
        compiler_params=pltpu.CompilerParams(
            collective_id=0, has_side_effects=True, vmem_limit_bytes=40 * 1024 * 1024
        ),
    )(*(pltpu.with_memory_space_constraint(x, pltpu.HBM) for x in args))


def solution(mesh):
    n, nh = mesh.shape["blk"], mesh.shape["head"]

    def on_device(q, k, v, tk, tv, block_image, gate, res, w):
        tok, cols = q.shape
        heads = cols // HD
        groups = n // heads
        td = res.shape[0]
        rows = heads * tok
        if groups == 2 and heads > 1 and td % LANES == 0 and tok % (2 * BS) == 0:
            return split_call(n, nh, q, k, v, tk, tv, block_image, gate, res, w)
        upad = -(-tk.shape[0] // LANES) * LANES
        vm = pl.BlockSpec(memory_space=pltpu.VMEM)
        anyw = pl.BlockSpec(memory_space=pl.ANY)
        dma = pltpu.SemaphoreType.DMA
        return pl.pallas_call(
            functools.partial(kernel, n, nh),
            out_shape=jax.ShapeDtypeStruct(res.shape, BF16),
            in_specs=[vm, vm, vm, vm, vm, pl.BlockSpec(memory_space=pltpu.SMEM), vm, anyw, anyw],
            out_specs=vm,
            scratch_shapes=[
                pltpu.VMEM((heads, tok // 2, LANES), BF16),
                pltpu.VMEM((heads, tok, LANES), BF16),
                pltpu.VMEM((heads, tok // 2, LANES), BF16),
                pltpu.VMEM((n, tok, LANES), BF16),
                pltpu.VMEM((upad, LANES), F32),
                pltpu.VMEM((rows, LANES), BF16),
                pltpu.VMEM((n * tok, LANES), BF16),
                pltpu.VMEM((n * tok, LANES), BF16),
                pltpu.VMEM((upad, LANES), BF16),
                pltpu.VMEM((upad, LANES), BF16),
                pltpu.VMEM((rows, LANES), F32),
                pltpu.VMEM((rows, LANES), F32),
                pltpu.VMEM((heads * nh, td // 2, LANES), BF16),
                pltpu.VMEM((heads * nh, td // 2, LANES), BF16),
                pltpu.VMEM((td, heads * nh * HD), BF16),
                pltpu.VMEM((w.shape[0] * nh, w.shape[1]), BF16),
                pltpu.VMEM(res.shape, BF16),
                dma((heads,)), dma((heads,)), dma((n,)), dma((n,)),
                dma((nh,)), dma((nh,)), dma((nh,)), dma((heads * nh,)), dma((heads * nh,)), dma((2,)),
            ],
            compiler_params=pltpu.CompilerParams(
                collective_id=0, has_side_effects=True, vmem_limit_bytes=60 * 1024 * 1024
            ),
        )(q, k, v, tk, tv, block_image, gate, res, w)

    placed = (
        P("blk", "head"), P("blk", "head"), P("blk", "head"), P(None, "head"), P(None, "head"),
        P(), P(), P(("blk", "head"), None), P("head", None),
    )
    return jax.shard_map(
        on_device, mesh=mesh, in_specs=placed, out_specs=P(("blk", "head"), None), check_vma=False
    )
```
